128 devices in a mesh: row: 8 (over y, core), col: 16 (over x, z).
Axes of the slice: x: 4, y: 4, z: 4, core: 2. Of those that a mesh axis runs over, the one named last changes fastest.
Arguments:
- matrix_in: float32 [4, 4096, 2, 8192], P(None, 'row', None, 'col'), as said below
- panel_start: int32 [1], replicated, may hold values from 0 to 29
Outputs:
- matrix_out: float32 [4, 4096, 2, 8192], P(None, 'row', None, 'col')
The draws below stay inside these ranges and needn't reach their ends.
Inputs may be any that keep to these rules, and one draw needn't show every extreme that they name: matrix_in is symmetric and positive definite.
All inputs are finite; a program needn't handle non-finite values.
Results may differ from the reference program's by a relative error of at most 0.0001.
Values sent between devices are 32-bit elements.
No kernel may reach another device: no remote copies, remote signals or barrier semaphores. Data moves between devices by JAX's collectives and lax.ppermute only.
A program may use at most 128 MiB of HBM per device.

```python
import jax
import jax.numpy as jnp
from jax import lax

ORDER = 16384
NB = 512
PANELS = 2
BLOCKS = 32
LOC_BR = 4
LOC_BC = 2


def draw_matrix_in(key, part):
    key_gen = jax.random.fold_in(key, 21)
    key_shift = jax.random.fold_in(key, 22)
    inner_count = max(2 * NB, ORDER // 16)
    generator = jax.random.truncated_normal(key_gen, -6.0, 6.0, (ORDER, inner_count), jnp.float32)
    shift = jax.random.uniform(key_shift, (ORDER,), jnp.float32, 0.4, 0.8)
    common = jnp.zeros((ORDER,), jnp.float32)
    scales = jnp.ones((ORDER,), jnp.float32)
    weight = 0.0
    gram = lax.dot_general(generator, generator, (((1,), (1,)), ((), ())), precision=lax.Precision.HIGHEST, preferred_element_type=jnp.float32)
    gram = gram * (1.0 / inner_count)
    gram = 0.5 * (gram + gram.T)
    matrix = gram + weight * common[:, None] * common[None, :] + jnp.diag(shift)
    matrix = scales[:, None] * matrix * scales[None, :]
    return matrix.reshape(LOC_BR, ORDER // LOC_BR, LOC_BC, ORDER // LOC_BC)


def setup_inputs(seed: int = 0) -> dict:
    arg_keys = jax.random.split(jax.random.key(seed), 3)
    matrix_in = draw_matrix_in(jax.random.fold_in(arg_keys[2], 71), 0)
    panel_start = jax.random.randint(arg_keys[1], (1,), 0, BLOCKS - 2).astype(jnp.int32)
    return dict(matrix_in=matrix_in, panel_start=panel_start)


def reference(matrix_in, panel_start):
    matrix = matrix_in.reshape(ORDER, ORDER)
    block_index = jnp.arange(ORDER, dtype=jnp.int32) // NB
    first_panel = panel_start[0].astype(jnp.int32)
    for panel_step in range(PANELS):
        panel = first_panel + panel_step
        offset = (panel * NB).astype(jnp.int32)
        zero_index = jnp.zeros((), jnp.int32)
        diag_block = lax.dynamic_slice(matrix, (offset, offset), (NB, NB))
        factor = jnp.linalg.cholesky(diag_block)
        column_strip = lax.dynamic_slice(matrix, (zero_index, offset), (ORDER, NB))
        solved = jax.scipy.linalg.solve_triangular(factor, column_strip.T, lower=True).T
        below_panel = (block_index > panel)[:, None]
        column = jnp.where(below_panel, solved, jnp.float32(0.0))
        product = lax.dot_general(column.astype(jnp.float32), column.astype(jnp.float32), (((1,), (1,)), ((), ())), precision=lax.Precision.HIGHEST, preferred_element_type=jnp.float32)
        matrix = matrix - product
        new_strip = jnp.where(below_panel, solved, column_strip)
        new_strip = lax.dynamic_update_slice(new_strip, factor, (offset, zero_index))
        matrix = lax.dynamic_update_slice(matrix, new_strip, (zero_index, offset))
    return matrix.reshape(matrix_in.shape)
```

```python
import jax
import jax.numpy as jnp
from jax import lax
from jax.experimental import pallas as pl
from jax.experimental.pallas import tpu as pltpu
from jax.sharding import PartitionSpec as P

F32 = jnp.float32
BF16 = jnp.bfloat16
T = 128
G = 8


def split2(x):
    hi = x.astype(BF16)
    return hi, (x - hi.astype(F32)).astype(BF16)


def split3(x):
    hi = x.astype(BF16)
    rest = x - hi.astype(F32)
    mid = rest.astype(BF16)
    return hi, mid, (rest - mid.astype(F32)).astype(BF16)


def dot(a, b, ca, cb):
    return lax.dot_general(a, b, (((ca,), (cb,)), ((), ())), preferred_element_type=F32)


def factor_block(block):
    groups = T // G
    sub = lax.broadcasted_iota(jnp.int32, (G, T), 0)
    lane = lax.broadcasted_iota(jnp.int32, (G, T), 1)
    upper = list(block)
    inv = [jnp.where(lane == sub + G * g, F32(1.0), F32(0.0)) for g in range(groups)]

    def over_lanes(x, i):
        return jnp.broadcast_to(x[:, i : i + 1], (G, T))

    def over_rows(x, i):
        return jnp.broadcast_to(x[i : i + 1, :], (G, T))

    for g in range(groups):
        a, w = upper[g], inv[g]
        cols = [over_lanes(a, G * g + i) for i in range(G)]
        scale, cross, rows_a, rows_w = [], {}, [], []
        for j in range(G):
            r = lax.rsqrt(over_rows(cols[j], j))
            scale.append(r)
            low = cols[j] * r
            for i in range(j + 1, G):
                cross[i, j] = over_rows(low, i)
                cols[i] = cols[i] - low * cross[i, j]
            u = over_rows(a, j) * r
            v = over_rows(w, j) * r
            rows_a.append(u)
            rows_w.append(v)
            below = jnp.where(sub > j, low, F32(0.0))
            a = jnp.where(sub == j, u, a - below * u)
            w = jnp.where(sub == j, v, w - below * v)
        upper[g], inv[g] = a, w
        for m in range(g + 1, groups):
            x, y = upper[m], inv[m]
            cols = [over_lanes(x, G * g + i) for i in range(G)]
            for j in range(G):
                low = cols[j] * scale[j]
                for i in range(j + 1, G):
                    cols[i] = cols[i] - low * cross[i, j]
                x = x - low * rows_a[j]
                y = y - low * rows_w[j]
            upper[m], inv[m] = x, y
    return upper, inv


def prod6(a, b, ca, cb):
    (ah, am, al), (bh, bm, bl) = a, b
    acc = dot(ah, bl, ca, cb) + dot(al, bh, ca, cb) + dot(am, bm, ca, cb)
    acc = acc + (dot(ah, bm, ca, cb) + dot(am, bh, ca, cb))
    return acc + dot(ah, bh, ca, cb)


def prod3(a, b, ca, cb):
    (ah, al), (bh, bl) = a, b
    return dot(ah, bl, ca, cb) + dot(al, bh, ca, cb) + dot(ah, bh, ca, cb)


def chol_kernel(q_ref, own_ref, near_ref, u_ref, w_ref, d_ref, uh, um, ul):
    n = d_ref.shape[0]
    width = n // 2
    parts = (uh, um, ul)
    slab, lanes = width // 8, width // 2
    for ref, mine in ((own_ref, 0), (near_ref, 1)):
        for s in range(4):
            source = lax.rem(q_ref[0] - 2 * s + 8, 8)
            source = source + mine * (1 - 2 * lax.rem(source, 2))
            for e in range(2 * (slab // G)):
                rows = source * slab + (e // 2) * G
                for m in range(3):
                    dest = pl.ds(pl.multiple_of(rows + (m // 2) * width, G), G)
                    first = (m > 0) * width + (e % 2) * lanes
                    d_ref[dest, first : first + lanes] = ref[s, e * 3 + m]
    row = lax.broadcasted_iota(jnp.int32, (T, T), 0)
    col = lax.broadcasted_iota(jnp.int32, (T, T), 1)

    def body(b, carry):
        own = pl.ds(pl.multiple_of(b * T, T), T)
        for at in range(n // T):
            rest = slice(at * T, n)

            @pl.when(b == at)
            def _():
                strip = d_ref[rest.start : rest.start + T, rest]
                if at:
                    done = slice(0, at * T)
                    here = slice(at * T, at * T + T)
                    strip = strip - prod6(
                        [p[done, here] for p in parts], [p[done, rest] for p in parts], 0, 0
                    )
                u_ref[rest.start : rest.start + T, rest] = strip

        block = u_ref[own, own]
        upper, inv = factor_block([block[G * g : G * g + G, :] for g in range(T // G)])
        upper = jnp.where(col >= row, jnp.concatenate(upper, 0), F32(0.0))
        inv = jnp.concatenate(inv, 0)
        w_ref[own, :] = inv
        u_ref[own, own] = upper
        for p, x in zip(parts, split3(upper)):
            p[own, own] = x
        for at in range(n // T - 1):
            here = slice(at * T, at * T + T)
            rest = slice(at * T + T, n)

            @pl.when(b == at)
            def _():
                solved = prod6(split3(w_ref[here, :]), split3(u_ref[here, rest]), 1, 0)
                u_ref[here, rest] = solved
                for p, x in zip(parts, split3(solved)):
                    p[here, rest] = x

        return carry

    lax.fori_loop(0, n // T, body, 0)


def chol(q, mine, partner, width):
    n = 2 * width
    return pl.pallas_call(
        chol_kernel,
        grid_spec=pltpu.PrefetchScalarGridSpec(
            num_scalar_prefetch=1,
            grid=(1,),
            in_specs=[pl.BlockSpec(mine.shape, lambda g, f: (0, 0, 0, 0))] * 2,
            out_specs=[
                pl.BlockSpec((n, n), lambda g, f: (0, 0)),
                pl.BlockSpec((n, T), lambda g, f: (0, 0)),
            ],
            scratch_shapes=[pltpu.VMEM((n, n), F32)] + [pltpu.VMEM((n, n), BF16)] * 3,
        ),
        out_shape=(jax.ShapeDtypeStruct((n, n), F32), jax.ShapeDtypeStruct((n, T), F32)),
        compiler_params=pltpu.CompilerParams(vmem_limit_bytes=48 * 2**20),
        name="chol",
    )(q, mine, partner)


def solve_kernel(flag_ref, u_ref, w_ref, b_ref, hi_ref, lo_ref, uh, ul, wh, wl, rest_ref):
    n = u_ref.shape[0]
    width = n // 2
    wide = 2 * T
    tile = pl.program_id(0)

    @pl.when(tile == 0)
    def _():
        uh[...], ul[...] = split2(u_ref[...])
        for b in range(n // wide):
            r0 = slice(b * wide, b * wide + T)
            r1 = slice(b * wide + T, b * wide + wide)
            w0, w1 = split3(w_ref[r0, :]), split3(w_ref[r1, :])
            cross = prod6(split3(u_ref[r0, r1]), w0, 0, 0)
            corner = -prod6(w1, split3(cross), 1, 0)
            zero = jnp.zeros((T, T), F32)
            top = jnp.concatenate([w_ref[r0, :], zero], 1)
            low = jnp.concatenate([corner, w_ref[r1, :]], 1)
            wh[b * wide : b * wide + wide, :], wl[b * wide : b * wide + wide, :] = split2(
                jnp.concatenate([top, low], 0)
            )

    for b in range(n // wide):
        own = slice(b * wide, b * wide + wide)
        rest = slice(b * wide + wide, n)
        src = rest_ref if b else b_ref
        sol = split2(prod3((wh[own, :], wl[own, :]), split2(src[own, :]), 1, 0))
        keep = flag_ref[tile, b * wide // width] > 0
        for ref, x in zip((hi_ref, lo_ref), sol):
            ref[own, :] = jnp.where(keep, x, jnp.zeros_like(x))
        if rest.start < n:
            rest_ref[rest, :] = src[rest, :] - prod3((uh[own, rest], ul[own, rest]), sol, 0, 0)


def solve(flags, u, w, rhs, width):
    n, cols = rhs.shape
    return pl.pallas_call(
        solve_kernel,
        grid_spec=pltpu.PrefetchScalarGridSpec(
            num_scalar_prefetch=1,
            grid=(cols // width,),
            in_specs=[
                pl.BlockSpec((n, n), lambda t, f: (0, 0)),
                pl.BlockSpec((n, T), lambda t, f: (0, 0)),
                pl.BlockSpec((n, width), lambda t, f: (0, t)),
            ],
            out_specs=[pl.BlockSpec((n, width), lambda t, f: (0, t))] * 2,
            scratch_shapes=[pltpu.VMEM((n, n), BF16)] * 2
            + [pltpu.VMEM((n, 2 * T), BF16)] * 2
            + [pltpu.VMEM((n, width), F32)],
        ),
        out_shape=[jax.ShapeDtypeStruct((n, cols), BF16)] * 2,
        compiler_params=pltpu.CompilerParams(vmem_limit_bytes=48 * 2**20),
        name="solve",
    )(flags, u, w, rhs)


ROWS = 256


def update_kernel(mode_ref, a_ref, rh_ref, rl_ref, ch_ref, cl_ref, u_ref, o_ref):
    step = pl.program_id(0)
    part = pl.program_id(1)
    n, width2 = ch_ref.shape
    width = width2 // 2
    lanes = width // T
    for j in range(2):
        mode = mode_ref[step, j]
        cols = slice(j * width, (j + 1) * width)

        def put(value, keep):
            for t in range(lanes):
                at = pl.ds(t * 2 + j, ROWS, stride=2 * lanes)
                piece = value[:, t * T : t * T + T]
                o_ref[at, :] = a_ref[at, :] - piece if keep else piece

        @pl.when(mode == 0)
        def _():
            acc = dot(rh_ref[...], cl_ref[:, cols], 0, 0) + dot(rl_ref[...], ch_ref[:, cols], 0, 0)
            put(acc + dot(rh_ref[...], ch_ref[:, cols], 0, 0), True)

        for p in range(2):
            rows = slice(p * width, (p + 1) * width)

            @pl.when(mode == 1 + p)
            def _():
                put((rh_ref[rows, :].astype(F32) + rl_ref[rows, :].astype(F32)).T, False)

            @pl.when(mode == 3 + p)
            def _():
                first = part * ROWS
                tri = u_ref[rows, pl.ds(pl.multiple_of(p * width + first, ROWS), ROWS)]
                r = lax.broadcasted_iota(jnp.int32, tri.shape, 0)
                s = lax.broadcasted_iota(jnp.int32, tri.shape, 1) + first
                put(jnp.where(s >= r, tri, F32(0.0)).T, False)


def update(modes, a, rh, rl, ch, cl, u):
    loc_rows, width, loc_cols, _ = a.shape
    n = u.shape[0]
    lanes = width // T
    flat = a.reshape(loc_rows, width, loc_cols, lanes, T).transpose(0, 1, 3, 2, 4).reshape(-1, T)
    parts = width // ROWS
    per = ROWS * loc_cols * lanes

    def slot(i, r, m):
        return (0, ((i % 2) * 2 + i // 2) * parts + r)

    out = pl.pallas_call(
        update_kernel,
        grid_spec=pltpu.PrefetchScalarGridSpec(
            num_scalar_prefetch=1,
            grid=(loc_rows, parts),
            in_specs=[
                pl.BlockSpec((per, T), lambda i, r, m: (i * parts + r, 0)),
                pl.BlockSpec((n, ROWS), slot),
                pl.BlockSpec((n, ROWS), slot),
                pl.BlockSpec((n, loc_cols * width), lambda i, r, m: (0, 0)),
                pl.BlockSpec((n, loc_cols * width), lambda i, r, m: (0, 0)),
                pl.BlockSpec((n, n), lambda i, r, m: (0, 0)),
            ],
            out_specs=pl.BlockSpec((per, T), lambda i, r, m: (i * parts + r, 0)),
        ),
        out_shape=jax.ShapeDtypeStruct(flat.shape, F32),
        compiler_params=pltpu.CompilerParams(vmem_limit_bytes=48 * 2**20),
        name="update",
    )(modes, flat, rh, rl, ch, cl, u)
    out = out.reshape(loc_rows, width, lanes, loc_cols, T).transpose(0, 1, 3, 2, 4)
    return out.reshape(a.shape)


def diagonal(x, y, k, q, c, rows_dev, cols_dev, width):
    k1 = k + 1
    oc, oc1 = k % cols_dev, k1 % cols_dev

    def block_of(panel, p):
        return lax.dynamic_slice(
            x, (panel * width, (p // cols_dev) * width), (width, width)
        )

    first = jnp.where(c == oc, block_of(0, k), block_of(1, k1))
    second = block_of(0, k1)
    home = c % rows_dev
    cand = jnp.where(q == home, first, second).reshape(rows_dev, width // rows_dev, width)

    def chunk(r):
        return lax.dynamic_index_in_dim(cand, r % rows_dev, 0, keepdims=False)

    recv = [chunk(q)]
    for s in range(1, rows_dev):
        pairs = [(r, (r + s) % rows_dev) for r in range(rows_dev)]
        recv.append(lax.ppermute(chunk(q + s), "row", pairs))
    diag, upper = recv[0], recv[0]
    for s in range(1, rows_dev):
        diag = jnp.where((q - home) % rows_dev == s, recv[s], diag)
        upper = jnp.where((q - home + 1) % rows_dev == s, recv[s], upper)
    slots = jnp.stack([jnp.where(c == oc, diag, upper), diag])
    rows = slots.shape[1]
    slots = slots.reshape(2, rows // G, G, 2, width // 2).transpose(1, 3, 0, 2, 4)
    got = lax.all_to_all(slots.reshape(cols_dev, 2, G, width // 2), "col", 0, 0)
    got, y = lax.optimization_barrier((got, y))

    def pick(p, slot):
        return lax.dynamic_index_in_dim(got, p, 0, keepdims=False)[slot]

    d = jnp.concatenate([pick(oc, 0), pick(oc1, 0), pick(oc1, 1)], 0)
    for step, count in ((1, 4), (4, cols_dev // 4)):
        ring = [d]
        for s in range(1, count):
            pairs = []
            for p in range(cols_dev):
                at = (p // step) % count
                pairs.append((p, p + ((at + s) % count - at) * step))
            ring.append(lax.ppermute(d, "col", pairs))
        d = jnp.stack(ring)
        at = (c // step) % count
        order = (at - jnp.arange(count)) % count
        d = jnp.stack([lax.dynamic_index_in_dim(d, order[i], 0, keepdims=False) for i in range(count)])
        d = d.reshape(-1, width // 2)
    parts = [d]
    for s in range(1, rows_dev // 2):
        pairs = [(r, (r + 2 * s) % rows_dev) for r in range(rows_dev)]
        parts.append(lax.ppermute(d, "row", pairs))
    mine = jnp.stack(parts).reshape(len(parts), -1, G, width // 2)
    partner = lax.ppermute(mine, "row", [(r, r ^ 1) for r in range(rows_dev)])
    return mine, partner, y


def per_device(matrix, panel_start):
    rows_dev, cols_dev = lax.axis_size("row"), lax.axis_size("col")
    q, c = lax.axis_index("row"), lax.axis_index("col")
    loc_rows, width, loc_cols, _ = matrix.shape
    both = ("row", "col")
    k = panel_start[0]
    k1 = k + 1

    strips = []
    for p in (k, k1):
        strip = lax.dynamic_index_in_dim(matrix, p // rows_dev, 0, keepdims=False)
        strips.append(jnp.where(q == p % rows_dev, strip, F32(0.0)))
    x = jnp.concatenate(strips, 0).reshape(2 * width, loc_cols * width)
    y = lax.psum_scatter(x, "row", scatter_dimension=0, tiled=True)
    piece = y.shape[0]
    half = piece // 2

    mine, partner, y = diagonal(x, y, k, q, c, rows_dev, cols_dev, width)
    u, w = chol(q.astype(jnp.int32)[None], mine, partner, width)

    cpart = lax.all_gather(y, "row", axis=0, tiled=True)

    late = c >= rows_dev
    send = (
        jnp.where(late, y[half:], y[:half]),
        jnp.where(late, y[:half], y[half:]),
    )
    recv = []
    for h in range(2):
        pairs = []
        for r in range(rows_dev):
            for s in range(cols_dev):
                flip = h if s < rows_dev else 1 - h
                pairs.append((r * cols_dev + s, (s % rows_dev) * cols_dev + 2 * r + flip))
        recv.append(lax.ppermute(send[h], both, pairs))
    even = c % 2 == 0
    z = jnp.concatenate(
        [jnp.where(even, recv[0], recv[1]), jnp.where(even, recv[1], recv[0])], 1
    )
    rpart = lax.all_gather(z, "col", axis=0, tiled=True)

    i = jnp.arange(loc_rows, dtype=jnp.int32)
    slot_rows = ((i // 2) + 2 * (i % 2)) * rows_dev + q
    glob_cols = jnp.arange(loc_cols, dtype=jnp.int32) * cols_dev + c
    panels = jnp.stack([k, k1])
    flags_r = (slot_rows[:, None] > panels[None, :]).astype(jnp.int32)
    flags_c = (glob_cols[:, None] > panels[None, :]).astype(jnp.int32)
    ch, cl = solve(flags_c, u, w, cpart, width)
    rh, rl = solve(flags_r, u, w, rpart, width)

    gr = (i * rows_dev + q)[:, None]
    gc = glob_cols[None, :]
    modes = jnp.where(
        gc == k,
        jnp.where(gr > k, 1, jnp.where(gr == k, 3, 0)),
        jnp.where(gc == k1, jnp.where(gr > k1, 2, jnp.where(gr == k1, 4, 0)), 0),
    ).astype(jnp.int32)
    return update(modes, matrix, rh, rl, ch, cl, u)


def solution(mesh):
    return jax.shard_map(
        per_device,
        mesh=mesh,
        in_specs=(P(None, "row", None, "col"), P()),
        out_specs=P(None, "row", None, "col"),
        check_vma=False,
    )
```

```python
import jax
import jax.numpy as jnp
from jax import lax
from jax.experimental import pallas as pl
from jax.experimental.pallas import tpu as pltpu
from jax.sharding import PartitionSpec as P

F32 = jnp.float32
BF16 = jnp.bfloat16
T = 128
G = 8


def split2(x):
    hi = x.astype(BF16)
    return hi, (x - hi.astype(F32)).astype(BF16)


def split3(x):
    hi = x.astype(BF16)
    rest = x - hi.astype(F32)
    mid = rest.astype(BF16)
    return hi, mid, (rest - mid.astype(F32)).astype(BF16)


def dot(a, b, ca, cb):
    return lax.dot_general(a, b, (((ca,), (cb,)), ((), ())), preferred_element_type=F32)


def factor_block(block):
    groups = T // G
    sub = lax.broadcasted_iota(jnp.int32, (G, T), 0)
    lane = lax.broadcasted_iota(jnp.int32, (G, T), 1)
    upper = list(block)
    inv = [jnp.where(lane == sub + G * g, F32(1.0), F32(0.0)) for g in range(groups)]

    def over_lanes(x, i):
        return jnp.broadcast_to(x[:, i : i + 1], (G, T))

    def over_rows(x, i):
        return jnp.broadcast_to(x[i : i + 1, :], (G, T))

    ahead = [over_lanes(upper[0], i) for i in range(G)]
    for g in range(groups):
        a, w = upper[g], inv[g]
        cols = ahead
        scale, cross, rows_a, rows_w = [], {}, [], []
        for j in range(G):
            r = lax.rsqrt(over_rows(cols[j], j))
            scale.append(r)
            low = cols[j] * r
            for i in range(j + 1, G):
                cross[i, j] = over_rows(low, i)
                cols[i] = cols[i] - low * cross[i, j]
            u = over_rows(a, j) * r
            v = over_rows(w, j) * r
            rows_a.append(u)
            rows_w.append(v)
            below = jnp.where(sub > j, low, F32(0.0))
            a = jnp.where(sub == j, u, a - below * u)
            w = jnp.where(sub == j, v, w - below * v)
        upper[g], inv[g] = a, w
        for m in range(g + 1, groups):
            x, y = upper[m], inv[m]
            cols = [over_lanes(x, G * g + i) for i in range(G)]
            if m == g + 1:
                ahead = [over_lanes(x, G * m + i) for i in range(G)]
            for j in range(G):
                low = cols[j] * scale[j]
                for i in range(j + 1, G):
                    cols[i] = cols[i] - low * cross[i, j]
                if m == g + 1:
                    ahead = [p - low * over_rows(low, i) for i, p in enumerate(ahead)]
                x = x - low * rows_a[j]
                y = y - low * rows_w[j]
            upper[m], inv[m] = x, y
    return upper, inv


def prod6(a, b, ca, cb):
    (ah, am, al), (bh, bm, bl) = a, b
    acc = dot(ah, bl, ca, cb) + dot(al, bh, ca, cb) + dot(am, bm, ca, cb)
    acc = acc + (dot(ah, bm, ca, cb) + dot(am, bh, ca, cb))
    return acc + dot(ah, bh, ca, cb)


def prod3(a, b, ca, cb):
    (ah, al), (bh, bl) = a, b
    return dot(ah, bl, ca, cb) + dot(al, bh, ca, cb) + dot(ah, bh, ca, cb)


def chol_kernel(q_ref, own_ref, near_ref, u_ref, w_ref, d_ref, uh, um, ul):
    n = d_ref.shape[0]
    width = n // 2
    parts = (uh, um, ul)
    slab, lanes = width // 8, width // 2
    for ref, mine in ((own_ref, 0), (near_ref, 1)):
        for s in range(4):
            source = lax.rem(q_ref[0] - 2 * s + 8, 8)
            source = source + mine * (1 - 2 * lax.rem(source, 2))
            for e in range(2 * (slab // G)):
                rows = source * slab + (e // 2) * G
                for m in range(3):
                    dest = pl.ds(pl.multiple_of(rows + (m // 2) * width, G), G)
                    first = (m > 0) * width + (e % 2) * lanes
                    d_ref[dest, first : first + lanes] = ref[s, e * 3 + m]
    row = lax.broadcasted_iota(jnp.int32, (T, T), 0)
    col = lax.broadcasted_iota(jnp.int32, (T, T), 1)

    def body(b, carry):
        own = pl.ds(pl.multiple_of(b * T, T), T)
        for at in range(n // T):
            rest = slice(at * T, n)

            @pl.when(b == at)
            def _():
                strip = d_ref[rest.start : rest.start + T, rest]
                if at:
                    done = slice(0, at * T)
                    here = slice(at * T, at * T + T)
                    strip = strip - prod6(
                        [p[done, here] for p in parts], [p[done, rest] for p in parts], 0, 0
                    )
                u_ref[rest.start : rest.start + T, rest] = strip

        block = u_ref[own, own]
        upper, inv = factor_block([block[G * g : G * g + G, :] for g in range(T // G)])
        upper = jnp.where(col >= row, jnp.concatenate(upper, 0), F32(0.0))
        inv = jnp.concatenate(inv, 0)
        w_ref[own, :] = inv
        u_ref[own, own] = upper
        for p, x in zip(parts, split3(upper)):
            p[own, own] = x
        for at in range(n // T - 1):
            here = slice(at * T, at * T + T)
            rest = slice(at * T + T, n)

            @pl.when(b == at)
            def _():
                solved = prod6(split3(w_ref[here, :]), split3(u_ref[here, rest]), 1, 0)
                u_ref[here, rest] = solved
                for p, x in zip(parts, split3(solved)):
                    p[here, rest] = x

        return carry

    lax.fori_loop(0, n // T, body, 0)


def chol(q, mine, partner, width):
    n = 2 * width
    return pl.pallas_call(
        chol_kernel,
        grid_spec=pltpu.PrefetchScalarGridSpec(
            num_scalar_prefetch=1,
            grid=(1,),
            in_specs=[pl.BlockSpec(mine.shape, lambda g, f: (0, 0, 0, 0))] * 2,
            out_specs=[
                pl.BlockSpec((n, n), lambda g, f: (0, 0)),
                pl.BlockSpec((n, T), lambda g, f: (0, 0)),
            ],
            scratch_shapes=[pltpu.VMEM((n, n), F32)] + [pltpu.VMEM((n, n), BF16)] * 3,
        ),
        out_shape=(jax.ShapeDtypeStruct((n, n), F32), jax.ShapeDtypeStruct((n, T), F32)),
        compiler_params=pltpu.CompilerParams(vmem_limit_bytes=48 * 2**20),
        name="chol",
    )(q, mine, partner)


def strip_kernel(at_ref, first_ref, second_ref, x_ref, *cand_refs):
    width = x_ref.shape[0] // 2
    lanes = width // T
    for p, ref in enumerate((first_ref, second_ref)):
        keep = at_ref[2 + p] > 0
        for j in range(2):
            for t in range(lanes):
                value = ref[pl.ds(t * 2 + j, width, stride=2 * lanes), :]
                cols = slice(j * width + t * T, j * width + t * T + T)
                x_ref[p * width : p * width + width, cols] = jnp.where(keep, value, F32(0.0))
    rows = cand_refs[0].shape[0]
    cols = pl.ds(pl.multiple_of(at_ref[5] * width, width), width)
    for s, ref in enumerate(cand_refs):
        chunk = lax.rem(at_ref[6] + s, len(cand_refs))
        ref[...] = x_ref[pl.ds(pl.multiple_of(at_ref[4] * width + chunk * rows, rows), rows), cols]


def strips(at, flat, width, rows_dev):
    per = width * 2 * (width // T)
    n = 2 * width
    piece = width // rows_dev
    return pl.pallas_call(
        strip_kernel,
        grid_spec=pltpu.PrefetchScalarGridSpec(
            num_scalar_prefetch=1,
            grid=(1,),
            in_specs=[
                pl.BlockSpec((per, T), lambda g, f: (f[0], 0)),
                pl.BlockSpec((per, T), lambda g, f: (f[1], 0)),
            ],
            out_specs=[pl.BlockSpec((n, n), lambda g, f: (0, 0))]
            + [pl.BlockSpec((piece, width), lambda g, f: (0, 0))] * rows_dev,
        ),
        out_shape=[jax.ShapeDtypeStruct((n, n), F32)]
        + [jax.ShapeDtypeStruct((piece, width), F32)] * rows_dev,
        compiler_params=pltpu.CompilerParams(vmem_limit_bytes=40 * 2**20),
        name="strips",
    )(at, flat, flat)


def finish_kernel(
    flag_ref, mode_ref, u_ref, w_ref, r_ref, c0, c1, c2, c3, a_ref, o_ref,
    uh, ul, wh, wl, rest_ref, rh, rl, ch, cl, c_ref, sems,
):
    n = u_ref.shape[0]
    width = n // 2
    wide = 2 * T
    lanes = width // T
    step = pl.program_id(0)
    slabs = (c0, c1, c2, c3)

    def slab_copy(s):
        chip = lax.rem(flag_ref[6, 0] - s + 4, 4)
        rows = pl.ds(pl.multiple_of(chip * wide, wide), wide)
        return pltpu.make_async_copy(slabs[s], c_ref.at[rows, :], sems.at[s])

    @pl.when(step == 0)
    def _():
        for s in range(4):
            slab_copy(s).start()
        uh[...], ul[...] = split2(u_ref[...])
        for b in range(n // wide):
            r0 = slice(b * wide, b * wide + T)
            r1 = slice(b * wide + T, b * wide + wide)
            w0, w1 = split3(w_ref[r0, :]), split3(w_ref[r1, :])
            cross = prod6(split3(u_ref[r0, r1]), w0, 0, 0)
            corner = -prod6(w1, split3(cross), 1, 0)
            zero = jnp.zeros((T, T), F32)
            top = jnp.concatenate([w_ref[r0, :], zero], 1)
            low = jnp.concatenate([corner, w_ref[r1, :]], 1)
            wh[b * wide : b * wide + wide, :], wl[b * wide : b * wide + wide, :] = split2(
                jnp.concatenate([top, low], 0)
            )

    def solve(b_ref, hi_ref, lo_ref, base, slot, at, size):
        cols = pl.ds(at, size)
        for b in range(n // wide):
            own = slice(b * wide, b * wide + wide)
            rest = slice(b * wide + wide, n)
            src = rest_ref if b else b_ref
            sol = split2(prod3((wh[own, :], wl[own, :]), split2(src[own, cols]), 1, 0))
            for ref, x in zip((hi_ref, lo_ref), sol):
                for e in range(size // width):
                    keep = flag_ref[base + slot + e, b * wide // width] > 0
                    piece = x[:, e * width : e * width + width]
                    where = pl.ds(pl.multiple_of((slot + e) * width, width), width)
                    ref[own, where] = jnp.where(keep, piece, jnp.zeros_like(piece))
            if rest.start < n:
                rest_ref[rest, cols] = src[rest, cols] - prod3((uh[own, rest], ul[own, rest]), sol, 0, 0)

    def solve_pair(b_ref, hi_ref, lo_ref, base, slot):
        first, second = flag_ref[base + slot, 0], flag_ref[base + slot + 1, 0]

        @pl.when(first + second == 2)
        def _():
            solve(b_ref, hi_ref, lo_ref, base, slot, 0, 2 * width)

        @pl.when(first + second == 1)
        def _():
            at = pl.multiple_of(second * width, width)
            solve(b_ref, hi_ref, lo_ref, base, slot + second, at, width)

    @pl.when(step < 2)
    def _():
        solve_pair(r_ref, rh, rl, 0, 2 * step)

    @pl.when(step == 2)
    def _():
        for s in range(4):
            slab_copy(s).wait()
        solve_pair(c_ref, ch, cl, 4, 0)

    @pl.when(step >= 3)
    def _():
        block = step - 3
        mine = pl.ds(pl.multiple_of((lax.rem(block, 2) * 2 + block // 2) * width, width), width)

        def put(j, value, keep):
            for t in range(lanes):
                at = pl.ds(t * 2 + j, width, stride=2 * lanes)
                piece = value[:, t * T : t * T + T]
                o_ref[at, :] = a_ref[at, :] - piece if keep else piece

        def product(cols):
            return prod3((rh[:, mine], rl[:, mine]), (ch[:, cols], cl[:, cols]), 0, 0)

        both = (mode_ref[block, 0] == 0) & (mode_ref[block, 1] == 0)

        @pl.when(both)
        def _():
            value = product(slice(0, 2 * width))
            for j in range(2):
                put(j, value[:, j * width : j * width + width], True)

        @pl.when(jnp.logical_not(both))
        def _():
            def column(j, carry):
                mode = mode_ref[block, j]

                @pl.when(mode == 0)
                def _():
                    put(j, product(pl.ds(pl.multiple_of(j * width, width), width)), True)

                @pl.when(mode == 5)
                def _():
                    for t in range(lanes):
                        at = pl.ds(t * 2 + j, width, stride=2 * lanes)
                        o_ref[at, :] = a_ref[at, :]

                panel = pl.multiple_of(lax.rem(mode + 1, 2) * width, width)
                rows = pl.ds(panel, width)

                @pl.when((mode == 1) | (mode == 2))
                def _():
                    put(j, (rh[rows, mine].astype(F32) + rl[rows, mine].astype(F32)).T, False)

                @pl.when((mode == 3) | (mode == 4))
                def _():
                    tri = u_ref[rows, rows]
                    r = lax.broadcasted_iota(jnp.int32, tri.shape, 0)
                    s = lax.broadcasted_iota(jnp.int32, tri.shape, 1)
                    put(j, jnp.where(s >= r, tri, F32(0.0)).T, False)

                return carry

            lax.fori_loop(0, 2, column, 0)


def finish(flags, modes, u, w, rpart, slabs, flat):
    n = u.shape[0]
    width = n // 2
    per = width * 2 * (width // T)
    loc_rows = flat.shape[0] // per
    once = pl.Buffered(1)

    def block(t, f, m):
        return (jnp.maximum(t - 3, 0), 0)

    return pl.pallas_call(
        finish_kernel,
        grid_spec=pltpu.PrefetchScalarGridSpec(
            num_scalar_prefetch=2,
            grid=(3 + loc_rows,),
            in_specs=[
                pl.BlockSpec((n, n), lambda t, f, m: (0, 0), pipeline_mode=once),
                pl.BlockSpec((n, T), lambda t, f, m: (0, 0), pipeline_mode=once),
                pl.BlockSpec((n, n), lambda t, f, m: (0, jnp.minimum(t, 1))),
            ]
            + [pl.BlockSpec(memory_space=pl.ANY)] * 4
            + [pl.BlockSpec((per, T), block)],
            out_specs=pl.BlockSpec((per, T), block),
            scratch_shapes=[pltpu.VMEM((n, n), BF16)] * 2
            + [pltpu.VMEM((n, 2 * T), BF16)] * 2
            + [pltpu.VMEM((n, n), F32)]
            + [pltpu.VMEM((n, 2 * n), BF16)] * 2
            + [pltpu.VMEM((n, n), BF16)] * 2
            + [pltpu.VMEM((n, n), F32), pltpu.SemaphoreType.DMA((4,))],
        ),
        out_shape=jax.ShapeDtypeStruct(flat.shape, F32),
        compiler_params=pltpu.CompilerParams(vmem_limit_bytes=58 * 2**20),
        name="finish",
    )(flags, modes, u, w, rpart, *slabs, flat)


def diagonal(chunks, y, k, q, c, rows_dev, cols_dev, width):
    k1 = k + 1
    oc, oc1 = k % cols_dev, k1 % cols_dev
    home = c % rows_dev
    recv = [chunks[0]]
    for s in range(1, rows_dev):
        pairs = [(r, (r + s) % rows_dev) for r in range(rows_dev)]
        recv.append(lax.ppermute(chunks[s], "row", pairs))
    diag, upper = recv[0], recv[0]
    for s in range(1, rows_dev):
        diag = jnp.where((q - home) % rows_dev == s, recv[s], diag)
        upper = jnp.where((q - home + 1) % rows_dev == s, recv[s], upper)
    slots = jnp.stack([jnp.where(c == oc, diag, upper), diag])
    rows = slots.shape[1]
    slots = slots.reshape(2, rows // G, G, 2, width // 2).transpose(1, 3, 0, 2, 4)
    got = lax.all_to_all(slots.reshape(cols_dev, 2, G, width // 2), "col", 0, 0)
    got, y = lax.optimization_barrier((got, y))

    def pick(p, slot):
        return lax.dynamic_index_in_dim(got, p, 0, keepdims=False)[slot]

    d = jnp.concatenate([pick(oc, 0), pick(oc1, 0), pick(oc1, 1)], 0)
    return lax.all_gather(d, "col", axis=0, tiled=True), y


def over_rows_of_devices(d, rows_dev, width):
    parts = [d]
    for s in range(1, rows_dev // 2):
        pairs = [(r, (r + 2 * s) % rows_dev) for r in range(rows_dev)]
        parts.append(lax.ppermute(d, "row", pairs))
    mine = jnp.stack(parts).reshape(len(parts), -1, G, width // 2)
    partner = lax.ppermute(mine, "row", [(r, r ^ 1) for r in range(rows_dev)])
    return mine, partner


def per_device(matrix, panel_start):
    rows_dev, cols_dev = lax.axis_size("row"), lax.axis_size("col")
    q, c = lax.axis_index("row"), lax.axis_index("col")
    loc_rows, width, loc_cols, _ = matrix.shape
    both = ("row", "col")
    k = panel_start[0]
    k1 = k + 1

    lanes = width // T
    flat = matrix.reshape(loc_rows, width, loc_cols, lanes, T).transpose(0, 1, 3, 2, 4)
    flat = flat.reshape(-1, T)
    oc = k % cols_dev
    diag_here = q == c % rows_dev
    at = jnp.stack(
        [
            k // rows_dev,
            k1 // rows_dev,
            (q == k % rows_dev).astype(jnp.int32),
            (q == k1 % rows_dev).astype(jnp.int32),
            jnp.where(diag_here & (c != oc), 1, 0),
            jnp.where(diag_here & (c == oc), k // cols_dev, k1 // cols_dev),
            q,
        ]
    ).astype(jnp.int32)
    x, *chunks = strips(at, flat, width, rows_dev)
    y = lax.psum_scatter(x, "row", scatter_dimension=0, tiled=True)
    piece = y.shape[0]
    half = piece // 2

    d, y = diagonal(chunks, y, k, q, c, rows_dev, cols_dev, width)

    late = c >= rows_dev
    send = (
        jnp.where(late, y[half:], y[:half]),
        jnp.where(late, y[:half], y[half:]),
    )
    recv = []
    for h in range(2):
        pairs = []
        for r in range(rows_dev):
            for s in range(cols_dev):
                flip = h if s < rows_dev else 1 - h
                pairs.append((r * cols_dev + s, (s % rows_dev) * cols_dev + 2 * r + flip))
        recv.append(lax.ppermute(send[h], both, pairs))

    d, recv[0], recv[1] = lax.optimization_barrier((d, recv[0], recv[1]))
    other = lax.ppermute(y, "row", [(r, r ^ 1) for r in range(rows_dev)])
    mine, partner = over_rows_of_devices(d, rows_dev, width)
    even = c % 2 == 0
    z = jnp.concatenate(
        [jnp.where(even, recv[0], recv[1]), jnp.where(even, recv[1], recv[0])], 1
    )
    with jax.named_scope("rows_gather"):
        rpart = lax.all_gather(z, "col", axis=0, tiled=True)
    odd = q % 2 == 1
    slab = jnp.concatenate([jnp.where(odd, other, y), jnp.where(odd, y, other)], 0)
    mine, partner, slab = lax.optimization_barrier((mine, partner, slab))
    slabs = [slab]
    for s in range(1, rows_dev // 2):
        pairs = [(r, (r + 2 * s) % rows_dev) for r in range(rows_dev)]
        slabs.append(lax.ppermute(slab, "row", pairs))
    u, w = chol(q.astype(jnp.int32)[None], mine, partner, width)

    i = jnp.arange(loc_rows, dtype=jnp.int32)
    slot_rows = ((i // 2) + 2 * (i % 2)) * rows_dev + q
    glob_cols = jnp.arange(loc_cols, dtype=jnp.int32) * cols_dev + c
    panels = jnp.stack([k, k1])
    flags_r = (slot_rows[:, None] > panels[None, :]).astype(jnp.int32)
    flags_c = (glob_cols[:, None] > panels[None, :]).astype(jnp.int32)
    chip = jnp.stack([q // 2, q // 2])[None].astype(jnp.int32)
    flags = jnp.concatenate([flags_r, flags_c, chip], 0)

    gr = (i * rows_dev + q)[:, None]
    gc = glob_cols[None, :]
    modes = jnp.where(
        gc == k,
        jnp.where(gr > k, 1, jnp.where(gr == k, 3, 5)),
        jnp.where(
            gc == k1,
            jnp.where(gr > k1, 2, jnp.where(gr == k1, 4, 5)),
            jnp.where((gr > k) & (gc > k), 0, 5),
        ),
    ).astype(jnp.int32)
    out = finish(flags, modes, u, w, rpart, slabs, flat)
    out = out.reshape(loc_rows, width, lanes, loc_cols, T).transpose(0, 1, 3, 2, 4)
    return out.reshape(matrix.shape)


def solution(mesh):
    return jax.shard_map(
        per_device,
        mesh=mesh,
        in_specs=(P(None, "row", None, "col"), P()),
        out_specs=P(None, "row", None, "col"),
        check_vma=False,
    )
```

```python
import jax
import jax.numpy as jnp
from jax import lax
from jax.experimental import pallas as pl
from jax.experimental.pallas import tpu as pltpu
from jax.sharding import PartitionSpec as P


F32 = jnp.float32
BF16 = jnp.bfloat16
T = 128
G = 8


def split2(x):
    hi = x.astype(BF16)
    return hi, (x - hi.astype(F32)).astype(BF16)


def split3(x):
    hi = x.astype(BF16)
    rest = x - hi.astype(F32)
    mid = rest.astype(BF16)
    return hi, mid, (rest - mid.astype(F32)).astype(BF16)


def dot(a, b, ca, cb):
    return lax.dot_general(a, b, (((ca,), (cb,)), ((), ())), preferred_element_type=F32)


def factor_block(block):
    groups = T // G
    sub = lax.broadcasted_iota(jnp.int32, (G, T), 0)
    lane = lax.broadcasted_iota(jnp.int32, (G, T), 1)
    upper = list(block)
    inv = [jnp.where(lane == sub + G * g, F32(1.0), F32(0.0)) for g in range(groups)]

    def over_lanes(x, i):
        return jnp.broadcast_to(x[:, i : i + 1], (G, T))

    def over_rows(x, i):
        return jnp.broadcast_to(x[i : i + 1, :], (G, T))

    ahead = [over_lanes(upper[0], i) for i in range(G)]
    for g in range(groups):
        a, w = upper[g], inv[g]
        cols = ahead
        scale, cross, rows_a, rows_w = [], {}, [], []
        for j in range(G):
            r = lax.rsqrt(over_rows(cols[j], j))
            scale.append(r)
            low = cols[j] * r
            for i in range(j + 1, G):
                cross[i, j] = over_rows(low, i)
                cols[i] = cols[i] - low * cross[i, j]
            u = over_rows(a, j) * r
            v = over_rows(w, j) * r
            rows_a.append(u)
            rows_w.append(v)
            below = jnp.where(sub > j, low, F32(0.0))
            a = jnp.where(sub == j, u, a - below * u)
            w = jnp.where(sub == j, v, w - below * v)
        upper[g], inv[g] = a, w
        for m in range(g + 1, groups):
            x, y = upper[m], inv[m]
            cols = [over_lanes(x, G * g + i) for i in range(G)]
            if m == g + 1:
                ahead = [over_lanes(x, G * m + i) for i in range(G)]
            for j in range(G):
                low = cols[j] * scale[j]
                for i in range(j + 1, G):
                    cols[i] = cols[i] - low * cross[i, j]
                if m == g + 1:
                    ahead = [p - low * over_rows(low, i) for i, p in enumerate(ahead)]
                x = x - low * rows_a[j]
                y = y - low * rows_w[j]
            upper[m], inv[m] = x, y
    return upper, inv


def prod6(a, b, ca, cb):
    (ah, am, al), (bh, bm, bl) = a, b
    acc = dot(ah, bl, ca, cb) + dot(al, bh, ca, cb) + dot(am, bm, ca, cb)
    acc = acc + (dot(ah, bm, ca, cb) + dot(am, bh, ca, cb))
    return acc + dot(ah, bh, ca, cb)


def prod3(a, b, ca, cb):
    (ah, al), (bh, bl) = a, b
    return dot(ah, bl, ca, cb) + dot(al, bh, ca, cb) + dot(ah, bh, ca, cb)


def chol_kernel(q_ref, own_ref, near_ref, u_ref, w_ref, d_ref, uh, um, ul):
    n = d_ref.shape[0]
    width = n // 2
    parts = (uh, um, ul)
    slab, lanes = width // 8, width // 2
    for ref, mine in ((own_ref, 0), (near_ref, 1)):
        for s in range(4):
            source = lax.rem(q_ref[0] - 2 * s + 8, 8)
            source = source + mine * (1 - 2 * lax.rem(source, 2))
            for e in range(2 * (slab // G)):
                rows = source * slab + (e // 2) * G
                for m in range(3):
                    dest = pl.ds(pl.multiple_of(rows + (m // 2) * width, G), G)
                    first = (m > 0) * width + (e % 2) * lanes
                    d_ref[dest, first : first + lanes] = ref[s, e * 3 + m]
    row = lax.broadcasted_iota(jnp.int32, (T, T), 0)
    col = lax.broadcasted_iota(jnp.int32, (T, T), 1)

    def body(b, carry):
        own = pl.ds(pl.multiple_of(b * T, T), T)
        for at in range(n // T):
            rest = slice(at * T, n)

            @pl.when(b == at)
            def _():
                strip = d_ref[rest.start : rest.start + T, rest]
                if at:
                    done = slice(0, at * T)
                    here = slice(at * T, at * T + T)
                    strip = strip - prod6(
                        [p[done, here] for p in parts], [p[done, rest] for p in parts], 0, 0
                    )
                u_ref[rest.start : rest.start + T, rest] = strip

        block = u_ref[own, own]
        upper, inv = factor_block([block[G * g : G * g + G, :] for g in range(T // G)])
        upper = jnp.where(col >= row, jnp.concatenate(upper, 0), F32(0.0))
        inv = jnp.concatenate(inv, 0)
        w_ref[own, :] = inv
        u_ref[own, own] = upper
        for p, x in zip(parts, split3(upper)):
            p[own, own] = x
        for at in range(n // T - 1):
            here = slice(at * T, at * T + T)
            rest = slice(at * T + T, n)

            @pl.when(b == at)
            def _():
                solved = prod6(split3(w_ref[here, :]), split3(u_ref[here, rest]), 1, 0)
                u_ref[here, rest] = solved
                for p, x in zip(parts, split3(solved)):
                    p[here, rest] = x

        return carry

    lax.fori_loop(0, n // T, body, 0)


def chol(q, mine, partner, width):
    n = 2 * width
    return pl.pallas_call(
        chol_kernel,
        grid_spec=pltpu.PrefetchScalarGridSpec(
            num_scalar_prefetch=1,
            grid=(1,),
            in_specs=[pl.BlockSpec(mine.shape, lambda g, f: (0, 0, 0, 0))] * 2,
            out_specs=[
                pl.BlockSpec((n, n), lambda g, f: (0, 0)),
                pl.BlockSpec((n, T), lambda g, f: (0, 0)),
            ],
            scratch_shapes=[pltpu.VMEM((n, n), F32)] + [pltpu.VMEM((n, n), BF16)] * 3,
        ),
        out_shape=(jax.ShapeDtypeStruct((n, n), F32), jax.ShapeDtypeStruct((n, T), F32)),
        compiler_params=pltpu.CompilerParams(vmem_limit_bytes=48 * 2**20),
        name="chol",
    )(q, mine, partner)


def strip_kernel(at_ref, first_ref, second_ref, x_ref, *cand_refs):
    width = x_ref.shape[0] // 2
    lanes = width // T
    for p, ref in enumerate((first_ref, second_ref)):
        keep = at_ref[2 + p] > 0
        for j in range(2):
            for t in range(lanes):
                value = ref[pl.ds(t * 2 + j, width, stride=2 * lanes), :]
                cols = slice(j * width + t * T, j * width + t * T + T)
                x_ref[p * width : p * width + width, cols] = jnp.where(keep, value, F32(0.0))
    rows = cand_refs[0].shape[0]
    cols = pl.ds(pl.multiple_of(at_ref[5] * width, width), width)
    for s, ref in enumerate(cand_refs):
        chunk = lax.rem(at_ref[6] + s, len(cand_refs))
        ref[...] = x_ref[pl.ds(pl.multiple_of(at_ref[4] * width + chunk * rows, rows), rows), cols]


def strips(at, flat, width, rows_dev):
    per = width * 2 * (width // T)
    n = 2 * width
    piece = width // rows_dev
    flat = pltpu.with_memory_space_constraint(flat, pltpu.HBM)
    return pl.pallas_call(
        strip_kernel,
        grid_spec=pltpu.PrefetchScalarGridSpec(
            num_scalar_prefetch=1,
            grid=(1,),
            in_specs=[
                pl.BlockSpec((per, T), lambda g, f: (f[0], 0)),
                pl.BlockSpec((per, T), lambda g, f: (f[1], 0)),
            ],
            out_specs=[pl.BlockSpec((n, n), lambda g, f: (0, 0))]
            + [pl.BlockSpec((piece, width), lambda g, f: (0, 0))] * rows_dev,
        ),
        out_shape=[jax.ShapeDtypeStruct((n, n), F32)]
        + [jax.ShapeDtypeStruct((piece, width), F32)] * rows_dev,
        compiler_params=pltpu.CompilerParams(vmem_limit_bytes=40 * 2**20),
        name="strips",
    )(at, flat, flat)


def finish_kernel(
    flag_ref, mode_ref, u_ref, w_ref, r_ref, own_ref, other_ref, a_ref, o_ref,
    uh, ul, wh, wl, rest_ref, rh, rl, ch, cl, c_ref, sems,
):
    n = u_ref.shape[0]
    width = n // 2
    wide = 2 * T
    lanes = width // T
    step = pl.program_id(0)
    q = flag_ref[6, 0]

    def slab_copy(s):
        source = lax.rem(q - 2 * (s // 2) + 8, 8)
        if s % 2:
            source = source + 1 - 2 * lax.rem(source, 2)
        rows = pl.ds(pl.multiple_of(source * T, T), T)
        ref = (own_ref, other_ref)[s % 2]
        return pltpu.make_async_copy(ref.at[s // 2], c_ref.at[rows, :], sems.at[s])

    @pl.when(step == 0)
    def _():
        for s in range(8):
            slab_copy(s).start()
        uh[...], ul[...] = split2(u_ref[...])
        for b in range(n // wide):
            r0 = slice(b * wide, b * wide + T)
            r1 = slice(b * wide + T, b * wide + wide)
            w0, w1 = split3(w_ref[r0, :]), split3(w_ref[r1, :])
            cross = prod6(split3(u_ref[r0, r1]), w0, 0, 0)
            corner = -prod6(w1, split3(cross), 1, 0)
            zero = jnp.zeros((T, T), F32)
            top = jnp.concatenate([w_ref[r0, :], zero], 1)
            low = jnp.concatenate([corner, w_ref[r1, :]], 1)
            wh[b * wide : b * wide + wide, :], wl[b * wide : b * wide + wide, :] = split2(
                jnp.concatenate([top, low], 0)
            )

    def solve(b_ref, hi_ref, lo_ref, base, slot, at, size):
        cols = pl.ds(at, size)
        for b in range(n // wide):
            own = slice(b * wide, b * wide + wide)
            rest = slice(b * wide + wide, n)
            src = rest_ref if b else b_ref
            sol = split2(prod3((wh[own, :], wl[own, :]), split2(src[own, cols]), 1, 0))
            for ref, x in zip((hi_ref, lo_ref), sol):
                for e in range(size // width):
                    keep = flag_ref[base + slot + e, b * wide // width] > 0
                    piece = x[:, e * width : e * width + width]
                    where = pl.ds(pl.multiple_of((slot + e) * width, width), width)
                    ref[own, where] = jnp.where(keep, piece, jnp.zeros_like(piece))
            if rest.start < n:
                rest_ref[rest, cols] = src[rest, cols] - prod3((uh[own, rest], ul[own, rest]), sol, 0, 0)

    def solve_pair(b_ref, hi_ref, lo_ref, base, slot):
        first, second = flag_ref[base + slot, 0], flag_ref[base + slot + 1, 0]

        @pl.when(first + second == 2)
        def _():
            solve(b_ref, hi_ref, lo_ref, base, slot, 0, 2 * width)

        @pl.when(first + second == 1)
        def _():
            at = pl.multiple_of(second * width, width)
            solve(b_ref, hi_ref, lo_ref, base, slot + second, at, width)

    @pl.when(step < 2)
    def _():
        solve_pair(r_ref, rh, rl, 0, 2 * step)

    @pl.when(step == 2)
    def _():
        for s in range(8):
            slab_copy(s).wait()
        solve_pair(c_ref, ch, cl, 4, 0)

    @pl.when(step >= 3)
    def _():
        block = step - 3
        mine = pl.ds(pl.multiple_of((lax.rem(block, 2) * 2 + block // 2) * width, width), width)

        def put(j, value, keep):
            for t in range(lanes):
                at = pl.ds(t * 2 + j, width, stride=2 * lanes)
                piece = value[:, t * T : t * T + T]
                o_ref[at, :] = a_ref[at, :] - piece if keep else piece

        def product(cols):
            return prod3((rh[:, mine], rl[:, mine]), (ch[:, cols], cl[:, cols]), 0, 0)

        both = (mode_ref[block, 0] == 0) & (mode_ref[block, 1] == 0)

        @pl.when(both)
        def _():
            value = product(slice(0, 2 * width))
            for j in range(2):
                put(j, value[:, j * width : j * width + width], True)

        @pl.when(jnp.logical_not(both))
        def _():
            def column(j, carry):
                mode = mode_ref[block, j]

                @pl.when(mode == 0)
                def _():
                    put(j, product(pl.ds(pl.multiple_of(j * width, width), width)), True)

                @pl.when(mode == 5)
                def _():
                    for t in range(lanes):
                        at = pl.ds(t * 2 + j, width, stride=2 * lanes)
                        o_ref[at, :] = a_ref[at, :]

                panel = pl.multiple_of(lax.rem(mode + 1, 2) * width, width)
                rows = pl.ds(panel, width)

                @pl.when((mode == 1) | (mode == 2))
                def _():
                    put(j, (rh[rows, mine].astype(F32) + rl[rows, mine].astype(F32)).T, False)

                @pl.when((mode == 3) | (mode == 4))
                def _():
                    tri = u_ref[rows, rows]
                    r = lax.broadcasted_iota(jnp.int32, tri.shape, 0)
                    s = lax.broadcasted_iota(jnp.int32, tri.shape, 1)
                    put(j, jnp.where(s >= r, tri, F32(0.0)).T, False)

                return carry

            lax.fori_loop(0, 2, column, 0)


def finish(flags, modes, u, w, rpart, own, other, flat):
    n = u.shape[0]
    width = n // 2
    per = width * 2 * (width // T)
    loc_rows = flat.shape[0] // per
    once = pl.Buffered(1)

    def block(t, f, m):
        return (jnp.maximum(t - 3, 0), 0)

    return pl.pallas_call(
        finish_kernel,
        grid_spec=pltpu.PrefetchScalarGridSpec(
            num_scalar_prefetch=2,
            grid=(3 + loc_rows,),
            in_specs=[
                pl.BlockSpec((n, n), lambda t, f, m: (0, 0), pipeline_mode=once),
                pl.BlockSpec((n, T), lambda t, f, m: (0, 0), pipeline_mode=once),
                pl.BlockSpec((n, n), lambda t, f, m: (0, jnp.minimum(t, 1))),
            ]
            + [pl.BlockSpec(memory_space=pl.ANY)] * 2
            + [pl.BlockSpec((per, T), block)],
            out_specs=pl.BlockSpec((per, T), block),
            scratch_shapes=[pltpu.VMEM((n, n), BF16)] * 2
            + [pltpu.VMEM((n, 2 * T), BF16)] * 2
            + [pltpu.VMEM((n, n), F32)]
            + [pltpu.VMEM((n, 2 * n), BF16)] * 2
            + [pltpu.VMEM((n, n), BF16)] * 2
            + [pltpu.VMEM((n, n), F32), pltpu.SemaphoreType.DMA((8,))],
        ),
        out_shape=jax.ShapeDtypeStruct(flat.shape, F32),
        compiler_params=pltpu.CompilerParams(vmem_limit_bytes=58 * 2**20),
        name="finish",
    )(flags, modes, u, w, rpart, own, other, flat)


def diagonal(chunks, k, q, c, rows_dev, cols_dev, width):
    oc = k % cols_dev
    home = c % rows_dev
    recv = [chunks[0]]
    for s in range(1, rows_dev):
        pairs = [(r, (r + s) % rows_dev) for r in range(rows_dev)]
        recv.append(lax.ppermute(chunks[s], "row", pairs))
    diag, upper = recv[0], recv[0]
    for s in range(1, rows_dev):
        diag = jnp.where((q - home) % rows_dev == s, recv[s], diag)
        upper = jnp.where((q - home + 1) % rows_dev == s, recv[s], upper)
    slots = jnp.stack([jnp.where(c == oc, diag, upper), diag])
    rows = slots.shape[1]
    slots = slots.reshape(2, rows // G, G, 2, width // 2).transpose(1, 3, 0, 2, 4)
    got = lax.all_to_all(slots.reshape(cols_dev, 2, G, width // 2), "col", 0, 0)

    return got


def gathered_over_cols(got, k, cols_dev):
    oc, oc1 = k % cols_dev, (k + 1) % cols_dev

    def pick(p, slot):
        return lax.dynamic_index_in_dim(got, p, 0, keepdims=False)[slot]

    d = jnp.concatenate([pick(oc, 0), pick(oc1, 0), pick(oc1, 1)], 0)
    return lax.all_gather(d, "col", axis=0, tiled=True)


def over_rows_of_devices(d, rows_dev, width):
    parts = [d]
    for s in range(1, rows_dev // 2):
        pairs = [(r, (r + 2 * s) % rows_dev) for r in range(rows_dev)]
        parts.append(lax.ppermute(d, "row", pairs))
    mine = jnp.stack(parts).reshape(len(parts), -1, G, width // 2)
    partner = lax.ppermute(mine, "row", [(r, r ^ 1) for r in range(rows_dev)])
    return mine, partner


def per_device(matrix, panel_start):
    rows_dev, cols_dev = lax.axis_size("row"), lax.axis_size("col")
    q, c = lax.axis_index("row"), lax.axis_index("col")
    loc_rows, width, loc_cols, _ = matrix.shape
    both = ("row", "col")
    k = panel_start[0]
    k1 = k + 1

    lanes = width // T
    flat = matrix.reshape(loc_rows, width, loc_cols, lanes, T).transpose(0, 1, 3, 2, 4)
    flat = flat.reshape(-1, T)
    oc = k % cols_dev
    diag_here = q == c % rows_dev
    at = jnp.stack(
        [
            k // rows_dev,
            k1 // rows_dev,
            (q == k % rows_dev).astype(jnp.int32),
            (q == k1 % rows_dev).astype(jnp.int32),
            jnp.where(diag_here & (c != oc), 1, 0),
            jnp.where(diag_here & (c == oc), k // cols_dev, k1 // cols_dev),
            q,
        ]
    ).astype(jnp.int32)
    x, *chunks = strips(at, flat, width, rows_dev)
    y = lax.psum_scatter(x, "row", scatter_dimension=0, tiled=True)
    piece = y.shape[0]
    half = piece // 2

    got = diagonal(chunks, k, q, c, rows_dev, cols_dev, width)
    got, y = lax.optimization_barrier((got, y))

    late = c >= rows_dev
    send = (
        jnp.where(late, y[half:], y[:half]),
        jnp.where(late, y[:half], y[half:]),
    )
    recv = []
    for h in range(2):
        pairs = []
        for r in range(rows_dev):
            for s in range(cols_dev):
                flip = h if s < rows_dev else 1 - h
                pairs.append((r * cols_dev + s, (s % rows_dev) * cols_dev + 2 * r + flip))
        recv.append(lax.ppermute(send[h], both, pairs))

    even = c % 2 == 0
    z = jnp.concatenate(
        [jnp.where(even, recv[0], recv[1]), jnp.where(even, recv[1], recv[0])], 1
    )
    rpart = lax.all_gather(z, "col", axis=0, tiled=True)
    own = [y]
    for s in range(1, rows_dev // 2):
        pairs = [(r, (r + 2 * s) % rows_dev) for r in range(rows_dev)]
        own.append(lax.ppermute(y, "row", pairs))
    got, z = lax.optimization_barrier((got, z))
    d = gathered_over_cols(got, k, cols_dev)
    mine, partner = over_rows_of_devices(d, rows_dev, width)
    own = jnp.stack(own)
    mine, partner, own = lax.optimization_barrier((mine, partner, own))
    other = lax.ppermute(own, "row", [(r, r ^ 1) for r in range(rows_dev)])
    u, w = chol(q.astype(jnp.int32)[None], mine, partner, width)

    i = jnp.arange(loc_rows, dtype=jnp.int32)
    slot_rows = ((i // 2) + 2 * (i % 2)) * rows_dev + q
    glob_cols = jnp.arange(loc_cols, dtype=jnp.int32) * cols_dev + c
    panels = jnp.stack([k, k1])
    flags_r = (slot_rows[:, None] > panels[None, :]).astype(jnp.int32)
    flags_c = (glob_cols[:, None] > panels[None, :]).astype(jnp.int32)
    chip = jnp.stack([q, q])[None].astype(jnp.int32)
    flags = jnp.concatenate([flags_r, flags_c, chip], 0)

    gr = (i * rows_dev + q)[:, None]
    gc = glob_cols[None, :]
    modes = jnp.where(
        gc == k,
        jnp.where(gr > k, 1, jnp.where(gr == k, 3, 5)),
        jnp.where(
            gc == k1,
            jnp.where(gr > k1, 2, jnp.where(gr == k1, 4, 5)),
            jnp.where((gr > k) & (gc > k), 0, 5),
        ),
    ).astype(jnp.int32)
    out = finish(flags, modes, u, w, rpart, own, other, flat)
    out = out.reshape(loc_rows, width, lanes, loc_cols, T).transpose(0, 1, 3, 2, 4)
    return out.reshape(matrix.shape)


def solution(mesh):
    return jax.shard_map(
        per_device,
        mesh=mesh,
        in_specs=(P(None, "row", None, "col"), P()),
        out_specs=P(None, "row", None, "col"),
        check_vma=False,
    )
```

```python
import jax
import jax.numpy as jnp
from jax import lax
from jax.experimental import pallas as pl
from jax.experimental.pallas import tpu as pltpu
from jax.sharding import PartitionSpec as P


F32 = jnp.float32
BF16 = jnp.bfloat16
T = 128
G = 8


def split2(x):
    hi = x.astype(BF16)
    return hi, (x - hi.astype(F32)).astype(BF16)


def split3(x):
    hi = x.astype(BF16)
    rest = x - hi.astype(F32)
    mid = rest.astype(BF16)
    return hi, mid, (rest - mid.astype(F32)).astype(BF16)


def dot(a, b, ca, cb):
    return lax.dot_general(a, b, (((ca,), (cb,)), ((), ())), preferred_element_type=F32)


def factor_block(block):
    groups = T // G
    sub = lax.broadcasted_iota(jnp.int32, (G, T), 0)
    lane = lax.broadcasted_iota(jnp.int32, (G, T), 1)
    upper = list(block)
    inv = [jnp.where(lane == sub + G * g, F32(1.0), F32(0.0)) for g in range(groups)]

    def over_lanes(x, i):
        return jnp.broadcast_to(x[:, i : i + 1], (G, T))

    def over_rows(x, i):
        return jnp.broadcast_to(x[i : i + 1, :], (G, T))

    ahead = [over_lanes(upper[0], i) for i in range(G)]
    for g in range(groups):
        a, w = upper[g], inv[g]
        cols = ahead
        scale, cross, rows_a, rows_w = [], {}, [], []
        for j in range(G):
            r = lax.rsqrt(over_rows(cols[j], j))
            scale.append(r)
            low = cols[j] * r
            for i in range(j + 1, G):
                cross[i, j] = over_rows(low, i)
                cols[i] = cols[i] - low * cross[i, j]
            u = over_rows(a, j) * r
            v = over_rows(w, j) * r
            rows_a.append(u)
            rows_w.append(v)
            below = jnp.where(sub > j, low, F32(0.0))
            a = jnp.where(sub == j, u, a - below * u)
            w = jnp.where(sub == j, v, w - below * v)
        upper[g], inv[g] = a, w
        for m in range(g + 1, groups):
            x, y = upper[m], inv[m]
            cols = [over_lanes(x, G * g + i) for i in range(G)]
            if m == g + 1:
                ahead = [over_lanes(x, G * m + i) for i in range(G)]
            for j in range(G):
                low = cols[j] * scale[j]
                for i in range(j + 1, G):
                    cols[i] = cols[i] - low * cross[i, j]
                if m == g + 1:
                    ahead = [p - low * over_rows(low, i) for i, p in enumerate(ahead)]
                x = x - low * rows_a[j]
                y = y - low * rows_w[j]
            upper[m], inv[m] = x, y
    return upper, inv


def prod6(a, b, ca, cb):
    (ah, am, al), (bh, bm, bl) = a, b
    acc = dot(ah, bl, ca, cb) + dot(al, bh, ca, cb) + dot(am, bm, ca, cb)
    acc = acc + (dot(ah, bm, ca, cb) + dot(am, bh, ca, cb))
    return acc + dot(ah, bh, ca, cb)


def prod3(a, b, ca, cb):
    (ah, al), (bh, bl) = a, b
    return dot(ah, bl, ca, cb) + dot(al, bh, ca, cb) + dot(ah, bh, ca, cb)


def chol_kernel(q_ref, own_ref, near_ref, u_ref, w_ref, d_ref, uh, um, ul):
    n = d_ref.shape[0]
    width = n // 2
    parts = (uh, um, ul)
    slab, lanes = width // 8, width // 2
    for ref, mine in ((own_ref, 0), (near_ref, 1)):
        for s in range(4):
            source = lax.rem(q_ref[0] - 2 * s + 8, 8)
            source = source + mine * (1 - 2 * lax.rem(source, 2))
            for e in range(2 * (slab // G)):
                rows = source * slab + (e // 2) * G
                for m in range(3):
                    dest = pl.ds(pl.multiple_of(rows + (m // 2) * width, G), G)
                    first = (m > 0) * width + (e % 2) * lanes
                    d_ref[dest, first : first + lanes] = ref[s, e * 3 + m]
    row = lax.broadcasted_iota(jnp.int32, (T, T), 0)
    col = lax.broadcasted_iota(jnp.int32, (T, T), 1)

    def body(b, carry):
        own = pl.ds(pl.multiple_of(b * T, T), T)
        for at in range(n // T):
            rest = slice(at * T, n)

            @pl.when(b == at)
            def _():
                strip = d_ref[rest.start : rest.start + T, rest]
                if at:
                    done = slice(0, at * T)
                    here = slice(at * T, at * T + T)
                    strip = strip - prod6(
                        [p[done, here] for p in parts], [p[done, rest] for p in parts], 0, 0
                    )
                u_ref[rest.start : rest.start + T, rest] = strip

        block = u_ref[own, own]
        upper, inv = factor_block([block[G * g : G * g + G, :] for g in range(T // G)])
        upper = jnp.where(col >= row, jnp.concatenate(upper, 0), F32(0.0))
        inv = jnp.concatenate(inv, 0)
        w_ref[own, :] = inv
        u_ref[own, own] = upper
        for p, x in zip(parts, split3(upper)):
            p[own, own] = x
        for at in range(n // T - 1):
            here = slice(at * T, at * T + T)
            rest = slice(at * T + T, n)

            @pl.when(b == at)
            def _():
                solved = prod6(split3(w_ref[here, :]), split3(u_ref[here, rest]), 1, 0)
                u_ref[here, rest] = solved
                for p, x in zip(parts, split3(solved)):
                    p[here, rest] = x

        return carry

    lax.fori_loop(0, n // T, body, 0)


def chol(q, mine, partner, width):
    n = 2 * width
    return pl.pallas_call(
        chol_kernel,
        grid_spec=pltpu.PrefetchScalarGridSpec(
            num_scalar_prefetch=1,
            grid=(1,),
            in_specs=[pl.BlockSpec(mine.shape, lambda g, f: (0, 0, 0, 0))] * 2,
            out_specs=[
                pl.BlockSpec((n, n), lambda g, f: (0, 0)),
                pl.BlockSpec((n, T), lambda g, f: (0, 0)),
            ],
            scratch_shapes=[pltpu.VMEM((n, n), F32)] + [pltpu.VMEM((n, n), BF16)] * 3,
        ),
        out_shape=(jax.ShapeDtypeStruct((n, n), F32), jax.ShapeDtypeStruct((n, T), F32)),
        compiler_params=pltpu.CompilerParams(vmem_limit_bytes=48 * 2**20),
        name="chol",
    )(q, mine, partner)


def strip_kernel(at_ref, first_ref, second_ref, x_ref, *cand_refs):
    width = x_ref.shape[0] // 2
    lanes = width // T
    for p, ref in enumerate((first_ref, second_ref)):
        keep = at_ref[2 + p] > 0
        for j in range(2):
            for t in range(lanes):
                value = ref[pl.ds(t * 2 + j, width, stride=2 * lanes), :]
                cols = slice(j * width + t * T, j * width + t * T + T)
                x_ref[p * width : p * width + width, cols] = jnp.where(keep, value, F32(0.0))
    rows = cand_refs[0].shape[0]
    cols = pl.ds(pl.multiple_of(at_ref[5] * width, width), width)
    for s, ref in enumerate(cand_refs):
        chunk = lax.rem(at_ref[6] + s, len(cand_refs))
        ref[...] = x_ref[pl.ds(pl.multiple_of(at_ref[4] * width + chunk * rows, rows), rows), cols]


def strips(at, flat, width, rows_dev):
    per = width * 2 * (width // T)
    n = 2 * width
    piece = width // rows_dev
    flat = pltpu.with_memory_space_constraint(flat, pltpu.HBM)
    return pl.pallas_call(
        strip_kernel,
        grid_spec=pltpu.PrefetchScalarGridSpec(
            num_scalar_prefetch=1,
            grid=(1,),
            in_specs=[
                pl.BlockSpec((per, T), lambda g, f: (f[0], 0)),
                pl.BlockSpec((per, T), lambda g, f: (f[1], 0)),
            ],
            out_specs=[pl.BlockSpec((n, n), lambda g, f: (0, 0))]
            + [pl.BlockSpec((piece, width), lambda g, f: (0, 0))] * rows_dev,
        ),
        out_shape=[jax.ShapeDtypeStruct((n, n), F32)]
        + [jax.ShapeDtypeStruct((piece, width), F32)] * rows_dev,
        compiler_params=pltpu.CompilerParams(vmem_limit_bytes=40 * 2**20),
        name="strips",
    )(at, flat, flat)


def finish_kernel(
    flag_ref, mode_ref, u_ref, w_ref, r_ref, own_ref, other_ref, a_ref, o_ref,
    uh, ul, wh, wl, rest_ref, rh, rl, ch, cl, c_ref, sems,
):
    n = u_ref.shape[0]
    width = n // 2
    wide = 2 * T
    lanes = width // T
    step = pl.program_id(0)
    q = flag_ref[6, 0]

    def slab_copy(s):
        source = lax.rem(q - 2 * (s // 2) + 8, 8)
        if s % 2:
            source = source + 1 - 2 * lax.rem(source, 2)
        rows = pl.ds(pl.multiple_of(source * T, T), T)
        ref = (own_ref, other_ref)[s % 2]
        return pltpu.make_async_copy(ref.at[s // 2], c_ref.at[rows, :], sems.at[s])

    @pl.when(step == 0)
    def _():
        for s in range(8):
            slab_copy(s).start()
        uh[...], ul[...] = split2(u_ref[...])
        for b in range(n // wide):
            r0 = slice(b * wide, b * wide + T)
            r1 = slice(b * wide + T, b * wide + wide)
            w0, w1 = split3(w_ref[r0, :]), split3(w_ref[r1, :])
            cross = prod6(split3(u_ref[r0, r1]), w0, 0, 0)
            corner = -prod6(w1, split3(cross), 1, 0)
            zero = jnp.zeros((T, T), F32)
            top = jnp.concatenate([w_ref[r0, :], zero], 1)
            low = jnp.concatenate([corner, w_ref[r1, :]], 1)
            wh[b * wide : b * wide + wide, :], wl[b * wide : b * wide + wide, :] = split2(
                jnp.concatenate([top, low], 0)
            )

    def solve(b_ref, hi_ref, lo_ref, base, slot, at, size):
        cols = pl.ds(at, size)
        for b in range(n // wide):
            own = slice(b * wide, b * wide + wide)
            rest = slice(b * wide + wide, n)
            src = rest_ref if b else b_ref
            sol = split2(prod3((wh[own, :], wl[own, :]), split2(src[own, cols]), 1, 0))
            for ref, x in zip((hi_ref, lo_ref), sol):
                for e in range(size // width):
                    keep = flag_ref[base + slot + e, b * wide // width] > 0
                    piece = x[:, e * width : e * width + width]
                    where = pl.ds(pl.multiple_of((slot + e) * width, width), width)
                    ref[own, where] = jnp.where(keep, piece, jnp.zeros_like(piece))
            if rest.start < n:
                rest_ref[rest, cols] = src[rest, cols] - prod3((uh[own, rest], ul[own, rest]), sol, 0, 0)

    def solve_pair(b_ref, hi_ref, lo_ref, base, slot):
        first, second = flag_ref[base + slot, 0], flag_ref[base + slot + 1, 0]

        @pl.when(first + second == 2)
        def _():
            solve(b_ref, hi_ref, lo_ref, base, slot, 0, 2 * width)

        @pl.when(first + second == 1)
        def _():
            at = pl.multiple_of(second * width, width)
            solve(b_ref, hi_ref, lo_ref, base, slot + second, at, width)

    @pl.when(step < 2)
    def _():
        solve_pair(r_ref, rh, rl, 0, 2 * step)

    @pl.when(step == 2)
    def _():
        for s in range(8):
            slab_copy(s).wait()
        solve_pair(c_ref, ch, cl, 4, 0)

    @pl.when(step >= 3)
    def _():
        block = step - 3
        mine = pl.ds(pl.multiple_of((lax.rem(block, 2) * 2 + block // 2) * width, width), width)

        def put(j, value, keep):
            for t in range(lanes):
                at = pl.ds(t * 2 + j, width, stride=2 * lanes)
                piece = value[:, t * T : t * T + T]
                o_ref[at, :] = a_ref[at, :] - piece if keep else piece

        def product(cols):
            return prod3((rh[:, mine], rl[:, mine]), (ch[:, cols], cl[:, cols]), 0, 0)

        both = (mode_ref[block, 0] == 0) & (mode_ref[block, 1] == 0)

        @pl.when(both)
        def _():
            value = product(slice(0, 2 * width))
            for j in range(2):
                put(j, value[:, j * width : j * width + width], True)

        @pl.when(jnp.logical_not(both))
        def _():
            def column(j, carry):
                mode = mode_ref[block, j]

                @pl.when(mode == 0)
                def _():
                    put(j, product(pl.ds(pl.multiple_of(j * width, width), width)), True)

                @pl.when(mode == 5)
                def _():
                    for t in range(lanes):
                        at = pl.ds(t * 2 + j, width, stride=2 * lanes)
                        o_ref[at, :] = a_ref[at, :]

                panel = pl.multiple_of(lax.rem(mode + 1, 2) * width, width)
                rows = pl.ds(panel, width)

                @pl.when((mode == 1) | (mode == 2))
                def _():
                    put(j, (rh[rows, mine].astype(F32) + rl[rows, mine].astype(F32)).T, False)

                @pl.when((mode == 3) | (mode == 4))
                def _():
                    tri = u_ref[rows, rows]
                    r = lax.broadcasted_iota(jnp.int32, tri.shape, 0)
                    s = lax.broadcasted_iota(jnp.int32, tri.shape, 1)
                    put(j, jnp.where(s >= r, tri, F32(0.0)).T, False)

                return carry

            lax.fori_loop(0, 2, column, 0)


def finish(flags, modes, u, w, rpart, own, other, flat):
    n = u.shape[0]
    width = n // 2
    per = width * 2 * (width // T)
    loc_rows = flat.shape[0] // per
    once = pl.Buffered(1)

    def block(t, f, m):
        return (jnp.maximum(t - 3, 0), 0)

    return pl.pallas_call(
        finish_kernel,
        grid_spec=pltpu.PrefetchScalarGridSpec(
            num_scalar_prefetch=2,
            grid=(3 + loc_rows,),
            in_specs=[
                pl.BlockSpec((n, n), lambda t, f, m: (0, 0), pipeline_mode=once),
                pl.BlockSpec((n, T), lambda t, f, m: (0, 0), pipeline_mode=once),
                pl.BlockSpec((n, n), lambda t, f, m: (0, jnp.minimum(t, 1))),
            ]
            + [pl.BlockSpec(memory_space=pl.ANY)] * 2
            + [pl.BlockSpec((per, T), block)],
            out_specs=pl.BlockSpec((per, T), block),
            scratch_shapes=[pltpu.VMEM((n, n), BF16)] * 2
            + [pltpu.VMEM((n, 2 * T), BF16)] * 2
            + [pltpu.VMEM((n, n), F32)]
            + [pltpu.VMEM((n, 2 * n), BF16)] * 2
            + [pltpu.VMEM((n, n), BF16)] * 2
            + [pltpu.VMEM((n, n), F32), pltpu.SemaphoreType.DMA((8,))],
        ),
        out_shape=jax.ShapeDtypeStruct(flat.shape, F32),
        compiler_params=pltpu.CompilerParams(vmem_limit_bytes=58 * 2**20),
        name="finish",
    )(flags, modes, u, w, rpart, own, other, flat)


def diagonal(chunks, k, q, c, rows_dev, cols_dev, width):
    k1 = k + 1
    oc, oc1 = k % cols_dev, k1 % cols_dev
    home = c % rows_dev
    recv = [chunks[0]]
    for s in range(1, rows_dev):
        pairs = [(r, (r + s) % rows_dev) for r in range(rows_dev)]
        recv.append(lax.ppermute(chunks[s], "row", pairs))
    diag, upper = recv[0], recv[0]
    for s in range(1, rows_dev):
        diag = jnp.where((q - home) % rows_dev == s, recv[s], diag)
        upper = jnp.where((q - home + 1) % rows_dev == s, recv[s], upper)
    slots = jnp.stack([jnp.where(c == oc, diag, upper), diag])
    rows = slots.shape[1]
    slots = slots.reshape(2, rows // G, G, 2, width // 2).transpose(1, 3, 0, 2, 4)
    got = lax.all_to_all(slots.reshape(cols_dev, 2, G, width // 2), "col", 0, 0)

    return got


def gathered_over_cols(got, k, cols_dev):
    oc, oc1 = k % cols_dev, (k + 1) % cols_dev

    def pick(p, slot):
        return lax.dynamic_index_in_dim(got, p, 0, keepdims=False)[slot]

    d = jnp.concatenate([pick(oc, 0), pick(oc1, 0), pick(oc1, 1)], 0)
    with jax.named_scope("d_cols"):
        return lax.all_gather(d, "col", axis=0, tiled=True)


def over_chips(x, rows_dev):
    parts = [x]
    for s in range(1, rows_dev // 2):
        pairs = [(r, (r + 2 * s) % rows_dev) for r in range(rows_dev)]
        parts.append(lax.ppermute(x, "row", pairs))
    return parts


def from_other_core(x, rows_dev):
    return lax.ppermute(x, "row", [(r, r ^ 1) for r in range(rows_dev)])


def per_device(matrix, panel_start):
    rows_dev, cols_dev = lax.axis_size("row"), lax.axis_size("col")
    q, c = lax.axis_index("row"), lax.axis_index("col")
    loc_rows, width, loc_cols, _ = matrix.shape
    both = ("row", "col")
    k = panel_start[0]
    k1 = k + 1

    lanes = width // T
    flat = matrix.reshape(loc_rows, width, loc_cols, lanes, T).transpose(0, 1, 3, 2, 4)
    flat = flat.reshape(-1, T)
    oc = k % cols_dev
    diag_here = q == c % rows_dev
    at = jnp.stack(
        [
            k // rows_dev,
            k1 // rows_dev,
            (q == k % rows_dev).astype(jnp.int32),
            (q == k1 % rows_dev).astype(jnp.int32),
            jnp.where(diag_here & (c != oc), 1, 0),
            jnp.where(diag_here & (c == oc), k // cols_dev, k1 // cols_dev),
            q,
        ]
    ).astype(jnp.int32)
    x, *chunks = strips(at, flat, width, rows_dev)
    y = lax.psum_scatter(x, "row", scatter_dimension=0, tiled=True)
    piece = y.shape[0]
    half = piece // 2

    got = diagonal(chunks, k, q, c, rows_dev, cols_dev, width)
    d = gathered_over_cols(got, k, cols_dev)
    d, y = lax.optimization_barrier((d, y))

    late = c >= rows_dev
    send = (
        jnp.where(late, y[half:], y[:half]),
        jnp.where(late, y[:half], y[half:]),
    )
    recv = []
    for h in range(2):
        pairs = []
        for r in range(rows_dev):
            for s in range(cols_dev):
                flip = h if s < rows_dev else 1 - h
                pairs.append((r * cols_dev + s, (s % rows_dev) * cols_dev + 2 * r + flip))
        recv.append(lax.ppermute(send[h], both, pairs))

    parts = over_chips(d, rows_dev)
    recv, parts, y = lax.optimization_barrier((recv, parts, y))
    even = c % 2 == 0
    z = jnp.concatenate(
        [jnp.where(even, recv[0], recv[1]), jnp.where(even, recv[1], recv[0])], 1
    )
    rpart = lax.all_gather(z, "col", axis=0, tiled=True)
    mine = jnp.stack(parts).reshape(len(parts), -1, G, width // 2)
    partner = from_other_core(mine, rows_dev)
    with jax.named_scope("c_shift"):
        own = over_chips(y, rows_dev)
    own = jnp.stack(own)
    mine, partner, own = lax.optimization_barrier((mine, partner, own))
    other = from_other_core(own, rows_dev)
    u, w = chol(q.astype(jnp.int32)[None], mine, partner, width)

    i = jnp.arange(loc_rows, dtype=jnp.int32)
    slot_rows = ((i // 2) + 2 * (i % 2)) * rows_dev + q
    glob_cols = jnp.arange(loc_cols, dtype=jnp.int32) * cols_dev + c
    panels = jnp.stack([k, k1])
    flags_r = (slot_rows[:, None] > panels[None, :]).astype(jnp.int32)
    flags_c = (glob_cols[:, None] > panels[None, :]).astype(jnp.int32)
    chip = jnp.stack([q, q])[None].astype(jnp.int32)
    flags = jnp.concatenate([flags_r, flags_c, chip], 0)

    gr = (i * rows_dev + q)[:, None]
    gc = glob_cols[None, :]
    modes = jnp.where(
        gc == k,
        jnp.where(gr > k, 1, jnp.where(gr == k, 3, 5)),
        jnp.where(
            gc == k1,
            jnp.where(gr > k1, 2, jnp.where(gr == k1, 4, 5)),
            jnp.where((gr > k) & (gc > k), 0, 5),
        ),
    ).astype(jnp.int32)
    out = finish(flags, modes, u, w, rpart, own, other, flat)
    out = out.reshape(loc_rows, width, lanes, loc_cols, T).transpose(0, 1, 3, 2, 4)
    return out.reshape(matrix.shape)


def solution(mesh):
    return jax.shard_map(
        per_device,
        mesh=mesh,
        in_specs=(P(None, "row", None, "col"), P()),
        out_specs=P(None, "row", None, "col"),
        check_vma=False,
    )
```

```python
import jax
import jax.numpy as jnp
from jax import lax
from jax.experimental import pallas as pl
from jax.experimental.pallas import tpu as pltpu
from jax.sharding import PartitionSpec as P


F32 = jnp.float32
BF16 = jnp.bfloat16
T = 128
G = 8


def split2(x):
    hi = x.astype(BF16)
    return hi, (x - hi.astype(F32)).astype(BF16)


def split3(x):
    hi = x.astype(BF16)
    rest = x - hi.astype(F32)
    mid = rest.astype(BF16)
    return hi, mid, (rest - mid.astype(F32)).astype(BF16)


def dot(a, b, ca, cb):
    return lax.dot_general(a, b, (((ca,), (cb,)), ((), ())), preferred_element_type=F32)


def factor_block(block):
    groups = T // G
    sub = lax.broadcasted_iota(jnp.int32, (G, T), 0)
    lane = lax.broadcasted_iota(jnp.int32, (G, T), 1)
    upper = list(block)
    inv = [jnp.where(lane == sub + G * g, F32(1.0), F32(0.0)) for g in range(groups)]

    def over_lanes(x, i):
        return jnp.broadcast_to(x[:, i : i + 1], (G, T))

    def over_rows(x, i):
        return jnp.broadcast_to(x[i : i + 1, :], (G, T))

    ahead = [over_lanes(upper[0], i) for i in range(G)]
    for g in range(groups):
        a, w = upper[g], inv[g]
        cols = ahead
        scale, cross, rows_a, rows_w = [], {}, [], []
        for j in range(G):
            r = lax.rsqrt(over_rows(cols[j], j))
            scale.append(r)
            low = cols[j] * r
            for i in range(j + 1, G):
                cross[i, j] = over_rows(low, i)
                cols[i] = cols[i] - low * cross[i, j]
            u = over_rows(a, j) * r
            v = over_rows(w, j) * r
            rows_a.append(u)
            rows_w.append(v)
            below = jnp.where(sub > j, low, F32(0.0))
            a = jnp.where(sub == j, u, a - below * u)
            w = jnp.where(sub == j, v, w - below * v)
        upper[g], inv[g] = a, w
        for m in range(g + 1, groups):
            x, y = upper[m], inv[m]
            cols = [over_lanes(x, G * g + i) for i in range(G)]
            if m == g + 1:
                ahead = [over_lanes(x, G * m + i) for i in range(G)]
            for j in range(G):
                low = cols[j] * scale[j]
                for i in range(j + 1, G):
                    cols[i] = cols[i] - low * cross[i, j]
                if m == g + 1:
                    ahead = [p - low * over_rows(low, i) for i, p in enumerate(ahead)]
                x = x - low * rows_a[j]
                y = y - low * rows_w[j]
            upper[m], inv[m] = x, y
    return upper, inv


def prod6(a, b, ca, cb):
    (ah, am, al), (bh, bm, bl) = a, b
    acc = dot(ah, bl, ca, cb) + dot(al, bh, ca, cb) + dot(am, bm, ca, cb)
    acc = acc + (dot(ah, bm, ca, cb) + dot(am, bh, ca, cb))
    return acc + dot(ah, bh, ca, cb)


def prod3(a, b, ca, cb):
    (ah, al), (bh, bl) = a, b
    return dot(ah, bl, ca, cb) + dot(al, bh, ca, cb) + dot(ah, bh, ca, cb)


def chol_kernel(q_ref, own_ref, near_ref, u_ref, w_ref, d_ref, uh, um, ul):
    n = d_ref.shape[0]
    width = n // 2
    parts = (uh, um, ul)
    slab, lanes = width // 8, width // 2
    for ref, mine in ((own_ref, 0), (near_ref, 1)):
        for s in range(4):
            source = lax.rem(q_ref[0] - 2 * s + 8, 8)
            source = source + mine * (1 - 2 * lax.rem(source, 2))
            for e in range(2 * (slab // G)):
                rows = source * slab + (e // 2) * G
                for m in range(3):
                    dest = pl.ds(pl.multiple_of(rows + (m // 2) * width, G), G)
                    first = (m > 0) * width + (e % 2) * lanes
                    d_ref[dest, first : first + lanes] = ref[s, e * 3 + m]
    row = lax.broadcasted_iota(jnp.int32, (T, T), 0)
    col = lax.broadcasted_iota(jnp.int32, (T, T), 1)

    def body(b, carry):
        own = pl.ds(pl.multiple_of(b * T, T), T)
        for at in range(n // T):
            rest = slice(at * T, n)

            @pl.when(b == at)
            def _():
                strip = d_ref[rest.start : rest.start + T, rest]
                if at:
                    done = slice(0, at * T)
                    here = slice(at * T, at * T + T)
                    strip = strip - prod6(
                        [p[done, here] for p in parts], [p[done, rest] for p in parts], 0, 0
                    )
                u_ref[rest.start : rest.start + T, rest] = strip

        block = u_ref[own, own]
        upper, inv = factor_block([block[G * g : G * g + G, :] for g in range(T // G)])
        upper = jnp.where(col >= row, jnp.concatenate(upper, 0), F32(0.0))
        inv = jnp.concatenate(inv, 0)
        w_ref[own, :] = inv
        u_ref[own, own] = upper
        for p, x in zip(parts, split3(upper)):
            p[own, own] = x
        for at in range(n // T - 1):
            here = slice(at * T, at * T + T)
            rest = slice(at * T + T, n)

            @pl.when(b == at)
            def _():
                solved = prod6(split3(w_ref[here, :]), split3(u_ref[here, rest]), 1, 0)
                u_ref[here, rest] = solved
                for p, x in zip(parts, split3(solved)):
                    p[here, rest] = x

        return carry

    lax.fori_loop(0, n // T, body, 0)


def chol(q, mine, partner, width):
    n = 2 * width
    return pl.pallas_call(
        chol_kernel,
        grid_spec=pltpu.PrefetchScalarGridSpec(
            num_scalar_prefetch=1,
            grid=(1,),
            in_specs=[pl.BlockSpec(mine.shape, lambda g, f: (0, 0, 0, 0))] * 2,
            out_specs=[
                pl.BlockSpec((n, n), lambda g, f: (0, 0)),
                pl.BlockSpec((n, T), lambda g, f: (0, 0)),
            ],
            scratch_shapes=[pltpu.VMEM((n, n), F32)] + [pltpu.VMEM((n, n), BF16)] * 3,
        ),
        out_shape=(jax.ShapeDtypeStruct((n, n), F32), jax.ShapeDtypeStruct((n, T), F32)),
        compiler_params=pltpu.CompilerParams(vmem_limit_bytes=48 * 2**20),
        name="chol",
    )(q, mine, partner)


def strip_kernel(at_ref, first_ref, second_ref, x_ref, *cand_refs):
    width = x_ref.shape[0] // 2
    lanes = width // T
    for p, ref in enumerate((first_ref, second_ref)):
        keep = at_ref[2 + p] > 0
        for j in range(2):
            for t in range(lanes):
                value = ref[pl.ds(t * 2 + j, width, stride=2 * lanes), :]
                cols = slice(j * width + t * T, j * width + t * T + T)
                x_ref[p * width : p * width + width, cols] = jnp.where(keep, value, F32(0.0))
    rows = cand_refs[0].shape[0]
    cols = pl.ds(pl.multiple_of(at_ref[5] * width, width), width)
    for s, ref in enumerate(cand_refs):
        chunk = lax.rem(at_ref[6] + s, len(cand_refs))
        ref[...] = x_ref[pl.ds(pl.multiple_of(at_ref[4] * width + chunk * rows, rows), rows), cols]


def strips(at, flat, width, rows_dev):
    per = width * 2 * (width // T)
    n = 2 * width
    piece = width // rows_dev
    flat = pltpu.with_memory_space_constraint(flat, pltpu.HBM)
    return pl.pallas_call(
        strip_kernel,
        grid_spec=pltpu.PrefetchScalarGridSpec(
            num_scalar_prefetch=1,
            grid=(1,),
            in_specs=[
                pl.BlockSpec((per, T), lambda g, f: (f[0], 0)),
                pl.BlockSpec((per, T), lambda g, f: (f[1], 0)),
            ],
            out_specs=[pl.BlockSpec((n, n), lambda g, f: (0, 0))]
            + [pl.BlockSpec((piece, width), lambda g, f: (0, 0))] * rows_dev,
        ),
        out_shape=[jax.ShapeDtypeStruct((n, n), F32)]
        + [jax.ShapeDtypeStruct((piece, width), F32)] * rows_dev,
        compiler_params=pltpu.CompilerParams(vmem_limit_bytes=40 * 2**20),
        name="strips",
    )(at, flat, flat)


def finish_kernel(
    flag_ref, mode_ref, u_ref, w_ref, r_ref, own_ref, other_ref, a_ref, o_ref,
    uh, ul, wh, wl, rest_ref, rh, rl, ch, cl, c_ref, sems,
):
    n = u_ref.shape[0]
    width = n // 2
    wide = 2 * T
    lanes = width // T
    step = pl.program_id(0)
    q = flag_ref[6, 0]

    def slab_copy(s):
        source = lax.rem(q - 2 * (s // 2) + 8, 8)
        if s % 2:
            source = source + 1 - 2 * lax.rem(source, 2)
        rows = pl.ds(pl.multiple_of(source * T, T), T)
        ref = (own_ref, other_ref)[s % 2]
        return pltpu.make_async_copy(ref.at[s // 2], c_ref.at[rows, :], sems.at[s])

    @pl.when(step == 0)
    def _():
        for s in range(8):
            slab_copy(s).start()
        uh[...], ul[...] = split2(u_ref[...])
        for b in range(n // wide):
            r0 = slice(b * wide, b * wide + T)
            r1 = slice(b * wide + T, b * wide + wide)
            w0, w1 = split3(w_ref[r0, :]), split3(w_ref[r1, :])
            cross = prod6(split3(u_ref[r0, r1]), w0, 0, 0)
            corner = -prod6(w1, split3(cross), 1, 0)
            zero = jnp.zeros((T, T), F32)
            top = jnp.concatenate([w_ref[r0, :], zero], 1)
            low = jnp.concatenate([corner, w_ref[r1, :]], 1)
            wh[b * wide : b * wide + wide, :], wl[b * wide : b * wide + wide, :] = split2(
                jnp.concatenate([top, low], 0)
            )

    def solve(b_ref, hi_ref, lo_ref, base, slot, at, size, turn):
        cols = pl.ds(at, size)
        count = n // wide

        def given(b):
            return b_ref[pl.ds(pl.multiple_of(lax.rem(turn + b, count) * wide, wide), wide), cols]

        for b in range(count):
            own = slice(b * wide, b * wide + wide)
            rest = slice(b * wide + wide, n)
            rhs = rest_ref[own, cols] if b else given(0)
            sol = split2(prod3((wh[own, :], wl[own, :]), split2(rhs), 1, 0))
            for ref, x in zip((hi_ref, lo_ref), sol):
                for e in range(size // width):
                    keep = flag_ref[base + slot + e, b * wide // width] > 0
                    piece = x[:, e * width : e * width + width]
                    where = pl.ds(pl.multiple_of((slot + e) * width, width), width)
                    ref[own, where] = jnp.where(keep, piece, jnp.zeros_like(piece))
            if rest.start < n:
                less = prod3((uh[own, rest], ul[own, rest]), sol, 0, 0)
                for e in range(b + 1, count):
                    rows = slice(e * wide, e * wide + wide)
                    before = rest_ref[rows, cols] if b else given(e)
                    rest_ref[rows, cols] = before - less[rows.start - rest.start : rows.stop - rest.start]

    def solve_pair(b_ref, hi_ref, lo_ref, base, slot, turn):
        first, second = flag_ref[base + slot, 0], flag_ref[base + slot + 1, 0]

        @pl.when(first + second == 2)
        def _():
            solve(b_ref, hi_ref, lo_ref, base, slot, 0, 2 * width, turn)

        @pl.when(first + second == 1)
        def _():
            at = pl.multiple_of(second * width, width)
            solve(b_ref, hi_ref, lo_ref, base, slot + second, at, width, turn)

    @pl.when(step < 2)
    def _():
        solve_pair(r_ref, rh, rl, 0, 2 * step, lax.div(q, 4) + 2 * step)

    @pl.when(step == 2)
    def _():
        for s in range(8):
            slab_copy(s).wait()
        solve_pair(c_ref, ch, cl, 4, 0, 0)

    @pl.when(step >= 3)
    def _():
        block = step - 3
        mine = pl.ds(pl.multiple_of((lax.rem(block, 2) * 2 + block // 2) * width, width), width)

        def put(j, value, keep):
            for t in range(lanes):
                at = pl.ds(t * 2 + j, width, stride=2 * lanes)
                piece = value[:, t * T : t * T + T]
                o_ref[at, :] = a_ref[at, :] - piece if keep else piece

        def product(cols):
            return prod3((rh[:, mine], rl[:, mine]), (ch[:, cols], cl[:, cols]), 0, 0)

        both = (mode_ref[block, 0] == 0) & (mode_ref[block, 1] == 0)

        @pl.when(both)
        def _():
            value = product(slice(0, 2 * width))
            for j in range(2):
                put(j, value[:, j * width : j * width + width], True)

        @pl.when(jnp.logical_not(both))
        def _():
            def column(j, carry):
                mode = mode_ref[block, j]

                @pl.when(mode == 0)
                def _():
                    put(j, product(pl.ds(pl.multiple_of(j * width, width), width)), True)

                @pl.when(mode == 5)
                def _():
                    for t in range(lanes):
                        at = pl.ds(t * 2 + j, width, stride=2 * lanes)
                        o_ref[at, :] = a_ref[at, :]

                panel = pl.multiple_of(lax.rem(mode + 1, 2) * width, width)
                rows = pl.ds(panel, width)

                @pl.when((mode == 1) | (mode == 2))
                def _():
                    put(j, (rh[rows, mine].astype(F32) + rl[rows, mine].astype(F32)).T, False)

                @pl.when((mode == 3) | (mode == 4))
                def _():
                    tri = u_ref[rows, rows]
                    r = lax.broadcasted_iota(jnp.int32, tri.shape, 0)
                    s = lax.broadcasted_iota(jnp.int32, tri.shape, 1)
                    put(j, jnp.where(s >= r, tri, F32(0.0)).T, False)

                return carry

            lax.fori_loop(0, 2, column, 0)


def finish(flags, modes, u, w, rpart, own, other, flat):
    n = u.shape[0]
    width = n // 2
    per = width * 2 * (width // T)
    loc_rows = flat.shape[0] // per
    once = pl.Buffered(1)

    def block(t, f, m):
        return (jnp.maximum(t - 3, 0), 0)

    return pl.pallas_call(
        finish_kernel,
        grid_spec=pltpu.PrefetchScalarGridSpec(
            num_scalar_prefetch=2,
            grid=(3 + loc_rows,),
            in_specs=[
                pl.BlockSpec((n, n), lambda t, f, m: (0, 0), pipeline_mode=once),
                pl.BlockSpec((n, T), lambda t, f, m: (0, 0), pipeline_mode=once),
                pl.BlockSpec((n, n), lambda t, f, m: (0, jnp.minimum(t, 1))),
            ]
            + [pl.BlockSpec(memory_space=pl.ANY)] * 2
            + [pl.BlockSpec((per, T), block)],
            out_specs=pl.BlockSpec((per, T), block),
            scratch_shapes=[pltpu.VMEM((n, n), BF16)] * 2
            + [pltpu.VMEM((n, 2 * T), BF16)] * 2
            + [pltpu.VMEM((n, n), F32)]
            + [pltpu.VMEM((n, 2 * n), BF16)] * 2
            + [pltpu.VMEM((n, n), BF16)] * 2
            + [pltpu.VMEM((n, n), F32), pltpu.SemaphoreType.DMA((8,))],
        ),
        out_shape=jax.ShapeDtypeStruct(flat.shape, F32),
        compiler_params=pltpu.CompilerParams(vmem_limit_bytes=58 * 2**20),
        name="finish",
    )(flags, modes, u, w, rpart, own, other, flat)


def diagonal(chunks, k, q, c, rows_dev, cols_dev, width):
    oc = k % cols_dev
    home = c % rows_dev
    recv = [chunks[0]]
    for s in range(1, rows_dev):
        pairs = [(r, (r + s) % rows_dev) for r in range(rows_dev)]
        recv.append(lax.ppermute(chunks[s], "row", pairs))
    diag, upper = recv[0], recv[0]
    for s in range(1, rows_dev):
        diag = jnp.where((q - home) % rows_dev == s, recv[s], diag)
        upper = jnp.where((q - home + 1) % rows_dev == s, recv[s], upper)
    slots = jnp.stack([jnp.where(c == oc, diag, upper), diag])
    rows = slots.shape[1]
    slots = slots.reshape(2, rows // G, G, 2, width // 2).transpose(1, 3, 0, 2, 4)
    got = lax.all_to_all(slots.reshape(cols_dev, 2, G, width // 2), "col", 0, 0)

    return got


def gathered_over_cols(got, k, cols_dev):
    oc, oc1 = k % cols_dev, (k + 1) % cols_dev

    def pick(p, slot):
        return lax.dynamic_index_in_dim(got, p, 0, keepdims=False)[slot]

    d = jnp.concatenate([pick(oc, 0), pick(oc1, 0), pick(oc1, 1)], 0)
    return lax.all_gather(d, "col", axis=0, tiled=True)


def over_rows_of_devices(d, rows_dev, width):
    parts = [d]
    for s in range(1, rows_dev // 2):
        pairs = [(r, (r + 2 * s) % rows_dev) for r in range(rows_dev)]
        parts.append(lax.ppermute(d, "row", pairs))
    mine = jnp.stack(parts).reshape(len(parts), -1, G, width // 2)
    partner = lax.ppermute(mine, "row", [(r, r ^ 1) for r in range(rows_dev)])
    return mine, partner


def per_device(matrix, panel_start):
    rows_dev, cols_dev = lax.axis_size("row"), lax.axis_size("col")
    q, c = lax.axis_index("row"), lax.axis_index("col")
    loc_rows, width, loc_cols, _ = matrix.shape
    both = ("row", "col")
    k = panel_start[0]
    k1 = k + 1

    lanes = width // T
    flat = matrix.reshape(loc_rows, width, loc_cols, lanes, T).transpose(0, 1, 3, 2, 4)
    flat = flat.reshape(-1, T)
    oc = k % cols_dev
    diag_here = q == c % rows_dev
    at = jnp.stack(
        [
            k // rows_dev,
            k1 // rows_dev,
            (q == k % rows_dev).astype(jnp.int32),
            (q == k1 % rows_dev).astype(jnp.int32),
            jnp.where(diag_here & (c != oc), 1, 0),
            jnp.where(diag_here & (c == oc), k // cols_dev, k1 // cols_dev),
            q,
        ]
    ).astype(jnp.int32)
    x, *chunks = strips(at, flat, width, rows_dev)
    y = lax.psum_scatter(x, "row", scatter_dimension=0, tiled=True)
    piece = y.shape[0]
    half = piece // 2

    got = diagonal(chunks, k, q, c, rows_dev, cols_dev, width)
    got, y = lax.optimization_barrier((got, y))

    late = c >= rows_dev
    send = (
        jnp.where(late, y[half:], y[:half]),
        jnp.where(late, y[:half], y[half:]),
    )
    recv = []
    for h in range(2):
        pairs = []
        for r in range(rows_dev):
            for s in range(cols_dev):
                flip = h if s < rows_dev else 1 - h
                to = (r // 2 + s // 4) % 4 * 4 + 2 * (r % 2) + flip
                pairs.append((r * cols_dev + s, (s % rows_dev) * cols_dev + to))
        recv.append(lax.ppermute(send[h], both, pairs))

    even = c % 2 == 0
    z = jnp.concatenate(
        [jnp.where(even, recv[0], recv[1]), jnp.where(even, recv[1], recv[0])], 1
    )
    rpart = lax.all_gather(z, "col", axis=0, tiled=True)
    own = [y]
    for s in range(1, rows_dev // 2):
        pairs = [(r, (r + 2 * s) % rows_dev) for r in range(rows_dev)]
        own.append(lax.ppermute(y, "row", pairs))
    got, z = lax.optimization_barrier((got, z))
    d = gathered_over_cols(got, k, cols_dev)
    mine, partner = over_rows_of_devices(d, rows_dev, width)
    own = jnp.stack(own)
    mine, partner, own = lax.optimization_barrier((mine, partner, own))
    other = lax.ppermute(own, "row", [(r, r ^ 1) for r in range(rows_dev)])
    u, w = chol(q.astype(jnp.int32)[None], mine, partner, width)

    i = jnp.arange(loc_rows, dtype=jnp.int32)
    slot_rows = ((i // 2) + 2 * (i % 2)) * rows_dev + q
    glob_cols = jnp.arange(loc_cols, dtype=jnp.int32) * cols_dev + c
    panels = jnp.stack([k, k1])
    flags_r = (slot_rows[:, None] > panels[None, :]).astype(jnp.int32)
    flags_c = (glob_cols[:, None] > panels[None, :]).astype(jnp.int32)
    chip = jnp.stack([q, q])[None].astype(jnp.int32)
    flags = jnp.concatenate([flags_r, flags_c, chip], 0)

    gr = (i * rows_dev + q)[:, None]
    gc = glob_cols[None, :]
    modes = jnp.where(
        gc == k,
        jnp.where(gr > k, 1, jnp.where(gr == k, 3, 5)),
        jnp.where(
            gc == k1,
            jnp.where(gr > k1, 2, jnp.where(gr == k1, 4, 5)),
            jnp.where((gr > k) & (gc > k), 0, 5),
        ),
    ).astype(jnp.int32)
    out = finish(flags, modes, u, w, rpart, own, other, flat)
    out = out.reshape(loc_rows, width, lanes, loc_cols, T).transpose(0, 1, 3, 2, 4)
    return out.reshape(matrix.shape)


def solution(mesh):
    return jax.shard_map(
        per_device,
        mesh=mesh,
        in_specs=(P(None, "row", None, "col"), P()),
        out_specs=P(None, "row", None, "col"),
        check_vma=False,
    )
```

```python
import jax
import jax.numpy as jnp
from jax import lax
from jax.experimental import pallas as pl
from jax.experimental.pallas import tpu as pltpu
from jax.sharding import PartitionSpec as P


F32 = jnp.float32
BF16 = jnp.bfloat16
T = 128
G = 8


def split2(x):
    hi = x.astype(BF16)
    return hi, (x - hi.astype(F32)).astype(BF16)


def split3(x):
    hi = x.astype(BF16)
    rest = x - hi.astype(F32)
    mid = rest.astype(BF16)
    return hi, mid, (rest - mid.astype(F32)).astype(BF16)


def dot(a, b, ca, cb):
    return lax.dot_general(a, b, (((ca,), (cb,)), ((), ())), preferred_element_type=F32)


def factor_block(block):
    groups = T // G
    sub = lax.broadcasted_iota(jnp.int32, (G, T), 0)
    lane = lax.broadcasted_iota(jnp.int32, (G, T), 1)
    upper = list(block)
    inv = [jnp.where(lane == sub + G * g, F32(1.0), F32(0.0)) for g in range(groups)]

    def over_lanes(x, i):
        return jnp.broadcast_to(x[:, i : i + 1], (G, T))

    def over_rows(x, i):
        return jnp.broadcast_to(x[i : i + 1, :], (G, T))

    ahead = [over_lanes(upper[0], i) for i in range(G)]
    for g in range(groups):
        a, w = upper[g], inv[g]
        cols = ahead
        scale, cross, rows_a, rows_w = [], {}, [], []
        for j in range(G):
            r = lax.rsqrt(over_rows(cols[j], j))
            scale.append(r)
            low = cols[j] * r
            for i in range(j + 1, G):
                cross[i, j] = over_rows(low, i)
                cols[i] = cols[i] - low * cross[i, j]
            u = over_rows(a, j) * r
            v = over_rows(w, j) * r
            rows_a.append(u)
            rows_w.append(v)
            below = jnp.where(sub > j, low, F32(0.0))
            a = jnp.where(sub == j, u, a - below * u)
            w = jnp.where(sub == j, v, w - below * v)
        upper[g], inv[g] = a, w
        for m in range(g + 1, groups):
            x, y = upper[m], inv[m]
            cols = [over_lanes(x, G * g + i) for i in range(G)]
            if m == g + 1:
                ahead = [over_lanes(x, G * m + i) for i in range(G)]
            for j in range(G):
                low = cols[j] * scale[j]
                for i in range(j + 1, G):
                    cols[i] = cols[i] - low * cross[i, j]
                if m == g + 1:
                    ahead = [p - low * over_rows(low, i) for i, p in enumerate(ahead)]
                x = x - low * rows_a[j]
                y = y - low * rows_w[j]
            upper[m], inv[m] = x, y
    return upper, inv


def prod6(a, b, ca, cb):
    (ah, am, al), (bh, bm, bl) = a, b
    acc = dot(ah, bl, ca, cb) + dot(al, bh, ca, cb) + dot(am, bm, ca, cb)
    acc = acc + (dot(ah, bm, ca, cb) + dot(am, bh, ca, cb))
    return acc + dot(ah, bh, ca, cb)


def prod3(a, b, ca, cb):
    (ah, al), (bh, bl) = a, b
    return dot(ah, bl, ca, cb) + dot(al, bh, ca, cb) + dot(ah, bh, ca, cb)


def chol_kernel(q_ref, own_ref, near_ref, u_ref, w_ref, d_ref, uh, um, ul):
    n = d_ref.shape[0]
    width = n // 2
    parts = (uh, um, ul)
    slab, lanes = width // 8, width // 2
    for ref, mine in ((own_ref, 0), (near_ref, 1)):
        for s in range(4):
            source = lax.rem(q_ref[0] - 2 * s + 8, 8)
            source = source + mine * (1 - 2 * lax.rem(source, 2))
            for e in range(2 * (slab // G)):
                rows = source * slab + (e // 2) * G
                for m in range(3):
                    dest = pl.ds(pl.multiple_of(rows + (m // 2) * width, G), G)
                    first = (m > 0) * width + (e % 2) * lanes
                    d_ref[dest, first : first + lanes] = ref[s, e * 3 + m]
    row = lax.broadcasted_iota(jnp.int32, (T, T), 0)
    col = lax.broadcasted_iota(jnp.int32, (T, T), 1)

    def body(b, carry):
        own = pl.ds(pl.multiple_of(b * T, T), T)
        for at in range(n // T):
            rest = slice(at * T, n)

            @pl.when(b == at)
            def _():
                strip = d_ref[rest.start : rest.start + T, rest]
                if at:
                    done = slice(0, at * T)
                    here = slice(at * T, at * T + T)
                    strip = strip - prod6(
                        [p[done, here] for p in parts], [p[done, rest] for p in parts], 0, 0
                    )
                u_ref[rest.start : rest.start + T, rest] = strip

        block = u_ref[own, own]
        upper, inv = factor_block([block[G * g : G * g + G, :] for g in range(T // G)])
        upper = jnp.where(col >= row, jnp.concatenate(upper, 0), F32(0.0))
        inv = jnp.concatenate(inv, 0)
        w_ref[own, :] = inv
        u_ref[own, own] = upper
        for p, x in zip(parts, split3(upper)):
            p[own, own] = x
        for at in range(n // T - 1):
            here = slice(at * T, at * T + T)
            rest = slice(at * T + T, n)

            @pl.when(b == at)
            def _():
                solved = prod6(split3(w_ref[here, :]), split3(u_ref[here, rest]), 1, 0)
                u_ref[here, rest] = solved
                for p, x in zip(parts, split3(solved)):
                    p[here, rest] = x

        return carry

    lax.fori_loop(0, n // T, body, 0)


def chol(q, mine, partner, width):
    n = 2 * width
    return pl.pallas_call(
        chol_kernel,
        grid_spec=pltpu.PrefetchScalarGridSpec(
            num_scalar_prefetch=1,
            grid=(1,),
            in_specs=[pl.BlockSpec(mine.shape, lambda g, f: (0, 0, 0, 0))] * 2,
            out_specs=[
                pl.BlockSpec((n, n), lambda g, f: (0, 0)),
                pl.BlockSpec((n, T), lambda g, f: (0, 0)),
            ],
            scratch_shapes=[pltpu.VMEM((n, n), F32)] + [pltpu.VMEM((n, n), BF16)] * 3,
        ),
        out_shape=(jax.ShapeDtypeStruct((n, n), F32), jax.ShapeDtypeStruct((n, T), F32)),
        compiler_params=pltpu.CompilerParams(vmem_limit_bytes=48 * 2**20),
        name="chol",
    )(q, mine, partner)


def strip_kernel(at_ref, first_ref, second_ref, x_ref, *cand_refs):
    width = x_ref.shape[0] // 2
    lanes = width // T
    for p, ref in enumerate((first_ref, second_ref)):
        keep = at_ref[2 + p] > 0
        for j in range(2):
            for t in range(lanes):
                value = ref[pl.ds(t * 2 + j, width, stride=2 * lanes), :]
                cols = slice(j * width + t * T, j * width + t * T + T)
                x_ref[p * width : p * width + width, cols] = jnp.where(keep, value, F32(0.0))
    rows = cand_refs[0].shape[0]
    cols = pl.ds(pl.multiple_of(at_ref[5] * width, width), width)
    for s, ref in enumerate(cand_refs):
        chunk = lax.rem(at_ref[6] + s, len(cand_refs))
        ref[...] = x_ref[pl.ds(pl.multiple_of(at_ref[4] * width + chunk * rows, rows), rows), cols]


def strips(at, flat, width, rows_dev):
    per = width * 2 * (width // T)
    n = 2 * width
    piece = width // rows_dev
    flat = pltpu.with_memory_space_constraint(flat, pltpu.HBM)
    return pl.pallas_call(
        strip_kernel,
        grid_spec=pltpu.PrefetchScalarGridSpec(
            num_scalar_prefetch=1,
            grid=(1,),
            in_specs=[
                pl.BlockSpec((per, T), lambda g, f: (f[0], 0)),
                pl.BlockSpec((per, T), lambda g, f: (f[1], 0)),
            ],
            out_specs=[pl.BlockSpec((n, n), lambda g, f: (0, 0))]
            + [pl.BlockSpec((piece, width), lambda g, f: (0, 0))] * rows_dev,
        ),
        out_shape=[jax.ShapeDtypeStruct((n, n), F32)]
        + [jax.ShapeDtypeStruct((piece, width), F32)] * rows_dev,
        compiler_params=pltpu.CompilerParams(vmem_limit_bytes=40 * 2**20),
        name="strips",
    )(at, flat, flat)


def finish_kernel(
    flag_ref, mode_ref, u_ref, w_ref, r_ref, own_ref, other_ref, a_ref, o_ref,
    uh, ul, wh, wl, rest_ref, rh, rl, ch, cl, c_ref, sems,
):
    n = u_ref.shape[0]
    width = n // 2
    wide = 2 * T
    lanes = width // T
    step = pl.program_id(0)
    q = flag_ref[6, 0]

    def slab_copy(s):
        source = lax.rem(q - 2 * (s // 2) + 8, 8)
        if s % 2:
            source = source + 1 - 2 * lax.rem(source, 2)
        rows = pl.ds(pl.multiple_of(source * T, T), T)
        ref = (own_ref, other_ref)[s % 2]
        return pltpu.make_async_copy(ref.at[s // 2], c_ref.at[rows, :], sems.at[s])

    @pl.when(step == 0)
    def _():
        for s in range(8):
            slab_copy(s).start()
        uh[...], ul[...] = split2(u_ref[...])
        for b in range(n // wide):
            r0 = slice(b * wide, b * wide + T)
            r1 = slice(b * wide + T, b * wide + wide)
            w0, w1 = split3(w_ref[r0, :]), split3(w_ref[r1, :])
            cross = prod6(split3(u_ref[r0, r1]), w0, 0, 0)
            corner = -prod6(w1, split3(cross), 1, 0)
            zero = jnp.zeros((T, T), F32)
            top = jnp.concatenate([w_ref[r0, :], zero], 1)
            low = jnp.concatenate([corner, w_ref[r1, :]], 1)
            wh[b * wide : b * wide + wide, :], wl[b * wide : b * wide + wide, :] = split2(
                jnp.concatenate([top, low], 0)
            )

    def solve(b_ref, hi_ref, lo_ref, base, slot, at, size, turn):
        cols = pl.ds(at, size)
        count = n // wide

        def given(b):
            return b_ref[pl.ds(pl.multiple_of(lax.rem(turn + b, count) * wide, wide), wide), cols]

        for b in range(count):
            own = slice(b * wide, b * wide + wide)
            rest = slice(b * wide + wide, n)
            rhs = rest_ref[own, cols] if b else given(0)
            sol = split2(prod3((wh[own, :], wl[own, :]), split2(rhs), 1, 0))
            for ref, x in zip((hi_ref, lo_ref), sol):
                for e in range(size // width):
                    keep = flag_ref[base + slot + e, b * wide // width] > 0
                    piece = x[:, e * width : e * width + width]
                    where = pl.ds(pl.multiple_of((slot + e) * width, width), width)
                    ref[own, where] = jnp.where(keep, piece, jnp.zeros_like(piece))
            if rest.start < n:
                less = prod3((uh[own, rest], ul[own, rest]), sol, 0, 0)
                for e in range(b + 1, count):
                    rows = slice(e * wide, e * wide + wide)
                    before = rest_ref[rows, cols] if b else given(e)
                    rest_ref[rows, cols] = before - less[rows.start - rest.start : rows.stop - rest.start]

    def solve_pair(b_ref, hi_ref, lo_ref, base, slot, turn):
        first, second = flag_ref[base + slot, 0], flag_ref[base + slot + 1, 0]

        @pl.when(first + second == 2)
        def _():
            solve(b_ref, hi_ref, lo_ref, base, slot, 0, 2 * width, turn)

        @pl.when(first + second == 1)
        def _():
            at = pl.multiple_of(second * width, width)
            solve(b_ref, hi_ref, lo_ref, base, slot + second, at, width, turn)

    @pl.when(step < 2)
    def _():
        solve_pair(r_ref, rh, rl, 0, 2 * step, lax.div(q, 4) + 2 * step)

    @pl.when(step == 2)
    def _():
        for s in range(8):
            slab_copy(s).wait()
        solve_pair(c_ref, ch, cl, 4, 0, 0)

    @pl.when(step >= 3)
    def _():
        block = step - 3
        mine = pl.ds(pl.multiple_of((lax.rem(block, 2) * 2 + block // 2) * width, width), width)

        def put(j, value, keep):
            for t in range(lanes):
                at = pl.ds(t * 2 + j, width, stride=2 * lanes)
                piece = value[:, t * T : t * T + T]
                o_ref[at, :] = a_ref[at, :] - piece if keep else piece

        def product(cols):
            return prod3((rh[:, mine], rl[:, mine]), (ch[:, cols], cl[:, cols]), 0, 0)

        both = (mode_ref[block, 0] == 0) & (mode_ref[block, 1] == 0)

        @pl.when(both)
        def _():
            value = product(slice(0, 2 * width))
            for j in range(2):
                put(j, value[:, j * width : j * width + width], True)

        @pl.when(jnp.logical_not(both))
        def _():
            def column(j, carry):
                mode = mode_ref[block, j]

                @pl.when(mode == 0)
                def _():
                    put(j, product(pl.ds(pl.multiple_of(j * width, width), width)), True)

                @pl.when(mode == 5)
                def _():
                    for t in range(lanes):
                        at = pl.ds(t * 2 + j, width, stride=2 * lanes)
                        o_ref[at, :] = a_ref[at, :]

                panel = pl.multiple_of(lax.rem(mode + 1, 2) * width, width)
                rows = pl.ds(panel, width)

                @pl.when((mode == 1) | (mode == 2))
                def _():
                    put(j, (rh[rows, mine].astype(F32) + rl[rows, mine].astype(F32)).T, False)

                @pl.when((mode == 3) | (mode == 4))
                def _():
                    tri = u_ref[rows, rows]
                    r = lax.broadcasted_iota(jnp.int32, tri.shape, 0)
                    s = lax.broadcasted_iota(jnp.int32, tri.shape, 1)
                    put(j, jnp.where(s >= r, tri, F32(0.0)).T, False)

                return carry

            lax.fori_loop(0, 2, column, 0)


def finish(flags, modes, u, w, rpart, own, other, flat):
    n = u.shape[0]
    width = n // 2
    per = width * 2 * (width // T)
    loc_rows = flat.shape[0] // per
    once = pl.Buffered(1)

    def block(t, f, m):
        return (jnp.maximum(t - 3, 0), 0)

    return pl.pallas_call(
        finish_kernel,
        grid_spec=pltpu.PrefetchScalarGridSpec(
            num_scalar_prefetch=2,
            grid=(3 + loc_rows,),
            in_specs=[
                pl.BlockSpec((n, n), lambda t, f, m: (0, 0), pipeline_mode=once),
                pl.BlockSpec((n, T), lambda t, f, m: (0, 0), pipeline_mode=once),
                pl.BlockSpec((n, n), lambda t, f, m: (0, jnp.minimum(t, 1))),
            ]
            + [pl.BlockSpec(memory_space=pl.ANY)] * 2
            + [pl.BlockSpec((per, T), block)],
            out_specs=pl.BlockSpec((per, T), block),
            scratch_shapes=[pltpu.VMEM((n, n), BF16)] * 2
            + [pltpu.VMEM((n, 2 * T), BF16)] * 2
            + [pltpu.VMEM((n, n), F32)]
            + [pltpu.VMEM((n, 2 * n), BF16)] * 2
            + [pltpu.VMEM((n, n), BF16)] * 2
            + [pltpu.VMEM((n, n), F32), pltpu.SemaphoreType.DMA((8,))],
        ),
        out_shape=jax.ShapeDtypeStruct(flat.shape, F32),
        compiler_params=pltpu.CompilerParams(vmem_limit_bytes=58 * 2**20),
        name="finish",
    )(flags, modes, u, w, rpart, own, other, flat)


def diagonal(chunks, k, q, c, rows_dev, cols_dev, width):
    k1 = k + 1
    oc, oc1 = k % cols_dev, k1 % cols_dev
    home = c % rows_dev
    recv = [chunks[0]]
    for s in range(1, rows_dev):
        pairs = [(r, (r + s) % rows_dev) for r in range(rows_dev)]
        recv.append(lax.ppermute(chunks[s], "row", pairs))
    diag, upper = recv[0], recv[0]
    for s in range(1, rows_dev):
        diag = jnp.where((q - home) % rows_dev == s, recv[s], diag)
        upper = jnp.where((q - home + 1) % rows_dev == s, recv[s], upper)
    slots = jnp.stack([jnp.where(c == oc, diag, upper), diag])
    rows = slots.shape[1]
    slots = slots.reshape(2, rows // G, G, 2, width // 2).transpose(1, 3, 0, 2, 4)
    got = lax.all_to_all(slots.reshape(cols_dev, 2, G, width // 2), "col", 0, 0)

    return got


def gathered_over_cols(got, k, cols_dev):
    oc, oc1 = k % cols_dev, (k + 1) % cols_dev

    def pick(p, slot):
        return lax.dynamic_index_in_dim(got, p, 0, keepdims=False)[slot]

    d = jnp.concatenate([pick(oc, 0), pick(oc1, 0), pick(oc1, 1)], 0)
    with jax.named_scope("d_cols"):
        return lax.all_gather(d, "col", axis=0, tiled=True)


def over_rows_of_devices(d, rows_dev, width):
    parts = [d]
    for s in range(1, rows_dev // 2):
        pairs = [(r, (r + 2 * s) % rows_dev) for r in range(rows_dev)]
        parts.append(lax.ppermute(d, "row", pairs))
    mine = jnp.stack(parts).reshape(len(parts), -1, G, width // 2)
    partner = lax.ppermute(mine, "row", [(r, r ^ 1) for r in range(rows_dev)])
    return mine, partner


def per_device(matrix, panel_start):
    rows_dev, cols_dev = lax.axis_size("row"), lax.axis_size("col")
    q, c = lax.axis_index("row"), lax.axis_index("col")
    loc_rows, width, loc_cols, _ = matrix.shape
    both = ("row", "col")
    k = panel_start[0]
    k1 = k + 1

    lanes = width // T
    flat = matrix.reshape(loc_rows, width, loc_cols, lanes, T).transpose(0, 1, 3, 2, 4)
    flat = flat.reshape(-1, T)
    oc = k % cols_dev
    diag_here = q == c % rows_dev
    at = jnp.stack(
        [
            k // rows_dev,
            k1 // rows_dev,
            (q == k % rows_dev).astype(jnp.int32),
            (q == k1 % rows_dev).astype(jnp.int32),
            jnp.where(diag_here & (c != oc), 1, 0),
            jnp.where(diag_here & (c == oc), k // cols_dev, k1 // cols_dev),
            q,
        ]
    ).astype(jnp.int32)
    x, *chunks = strips(at, flat, width, rows_dev)
    y = lax.psum_scatter(x, "row", scatter_dimension=0, tiled=True)
    piece = y.shape[0]
    half = piece // 2

    got = diagonal(chunks, k, q, c, rows_dev, cols_dev, width)
    d = gathered_over_cols(got, k, cols_dev)
    d, y = lax.optimization_barrier((d, y))

    late = c >= rows_dev
    send = (
        jnp.where(late, y[half:], y[:half]),
        jnp.where(late, y[:half], y[half:]),
    )
    recv = []
    for h in range(2):
        pairs = []
        for r in range(rows_dev):
            for s in range(cols_dev):
                flip = h if s < rows_dev else 1 - h
                to = (r // 2 + s // 4) % 4 * 4 + 2 * (r % 2) + flip
                pairs.append((r * cols_dev + s, (s % rows_dev) * cols_dev + to))
        recv.append(lax.ppermute(send[h], both, pairs))

    d, y, recv = lax.optimization_barrier((d, y, recv))
    even = c % 2 == 0
    z = jnp.concatenate(
        [jnp.where(even, recv[0], recv[1]), jnp.where(even, recv[1], recv[0])], 1
    )
    rpart = lax.all_gather(z, "col", axis=0, tiled=True)
    own = [y]
    for s in range(1, rows_dev // 2):
        pairs = [(r, (r + 2 * s) % rows_dev) for r in range(rows_dev)]
        with jax.named_scope("c_shift"):
            own.append(lax.ppermute(y, "row", pairs))
    mine, partner = over_rows_of_devices(d, rows_dev, width)
    own = jnp.stack(own)
    mine, partner, own = lax.optimization_barrier((mine, partner, own))
    other = lax.ppermute(own, "row", [(r, r ^ 1) for r in range(rows_dev)])
    u, w = chol(q.astype(jnp.int32)[None], mine, partner, width)

    i = jnp.arange(loc_rows, dtype=jnp.int32)
    slot_rows = ((i // 2) + 2 * (i % 2)) * rows_dev + q
    glob_cols = jnp.arange(loc_cols, dtype=jnp.int32) * cols_dev + c
    panels = jnp.stack([k, k1])
    flags_r = (slot_rows[:, None] > panels[None, :]).astype(jnp.int32)
    flags_c = (glob_cols[:, None] > panels[None, :]).astype(jnp.int32)
    chip = jnp.stack([q, q])[None].astype(jnp.int32)
    flags = jnp.concatenate([flags_r, flags_c, chip], 0)

    gr = (i * rows_dev + q)[:, None]
    gc = glob_cols[None, :]
    modes = jnp.where(
        gc == k,
        jnp.where(gr > k, 1, jnp.where(gr == k, 3, 5)),
        jnp.where(
            gc == k1,
            jnp.where(gr > k1, 2, jnp.where(gr == k1, 4, 5)),
            jnp.where((gr > k) & (gc > k), 0, 5),
        ),
    ).astype(jnp.int32)
    out = finish(flags, modes, u, w, rpart, own, other, flat)
    out = out.reshape(loc_rows, width, lanes, loc_cols, T).transpose(0, 1, 3, 2, 4)
    return out.reshape(matrix.shape)


def solution(mesh):
    return jax.shard_map(
        per_device,
        mesh=mesh,
        in_specs=(P(None, "row", None, "col"), P()),
        out_specs=P(None, "row", None, "col"),
        check_vma=False,
    )
```
